32 devices in a mesh: rep: 1 (over z), seq: 32 (over y, x, core).
Axes of the slice: x: 4, y: 4, z: 1, core: 2. Of those that a mesh axis runs over, the one named last changes fastest.
The devices are a block of a 4x4x8 slice.
Arguments:
- hidden: bfloat16 [64, 4096], P('rep')
- w_query: bfloat16 [4096, 4096], replicated
- w_key: bfloat16 [4096, 1024], replicated
- w_value: bfloat16 [4096, 1024], replicated
- w_out: bfloat16 [4096, 4096], P('seq')
- k_cache: bfloat16 [64, 2048, 8, 128], P('rep', 'seq')
- v_cache: bfloat16 [64, 2048, 8, 128], P('rep', 'seq')
- positions: int32 [64], P('rep')
Outputs:
- output 1: bfloat16 [64, 4096], P('rep')
- output 2: bfloat16 [64, 2048, 8, 128], P('rep', 'seq')
- output 3: bfloat16 [64, 2048, 8, 128], P('rep', 'seq')
All inputs are finite; a program needn't handle non-finite values.
Results may differ from the reference program's by a relative error of at most 0.00568872.
Values are sent between devices in bfloat16 or wider.
A program may use at most 768 MiB of HBM per device.

```python
import math
import jax
import jax.numpy as jnp
from jax import lax

D_MODEL = 4096
NUM_HEADS = 32
KV_HEADS = 8
HEAD_DIM = 128
BATCH_SIZE = 64
LOCAL_LEN = 64
SEQ_LEN = 2048


def query_shift(hidden, w_query):
    group_size = NUM_HEADS // KV_HEADS
    q_flat = jnp.dot(hidden, w_query, preferred_element_type=jnp.float32).astype(jnp.bfloat16).astype(jnp.float32)
    q_heads = q_flat.reshape(BATCH_SIZE, KV_HEADS, group_size, HEAD_DIM)
    gram_mat = jnp.einsum('bkgd,bkhd->bkgh', q_heads, q_heads)
    coeffs = jnp.linalg.solve(gram_mat, jnp.ones((BATCH_SIZE, KV_HEADS, group_size, 1), jnp.float32))
    score_drop = math.log(SEQ_LEN) - 1.0
    return -score_drop * HEAD_DIM ** 0.5 * jnp.einsum('bkgo,bkgd->bkd', coeffs, q_heads)


def setup_inputs(seed: int = 0, part: int = 0) -> dict:
    root = jax.random.key(seed)
    shared = jax.random.split(root, 4)
    part_keys = jax.random.split(jax.random.fold_in(root, part), 6)
    blocks = SEQ_LEN // LOCAL_LEN
    block_shape = (BATCH_SIZE, blocks, LOCAL_LEN, KV_HEADS, HEAD_DIM)
    cache_shape = (BATCH_SIZE, SEQ_LEN, KV_HEADS, HEAD_DIM)
    q_width = NUM_HEADS * HEAD_DIM
    kv_width = KV_HEADS * HEAD_DIM
    hidden = jax.random.normal(part_keys[0], (BATCH_SIZE, D_MODEL), jnp.float32).astype(jnp.bfloat16)
    w_query = (jax.random.normal(shared[0], (D_MODEL, q_width), jnp.float32) * D_MODEL ** -0.5).astype(jnp.bfloat16)
    w_key = (jax.random.normal(shared[1], (D_MODEL, kv_width), jnp.float32) * D_MODEL ** -0.5).astype(jnp.bfloat16)
    w_value = (jax.random.normal(shared[2], (D_MODEL, kv_width), jnp.float32) * D_MODEL ** -0.5).astype(jnp.bfloat16)
    w_out = (jax.random.normal(shared[3], (q_width, D_MODEL), jnp.float32) * q_width ** -0.5).astype(jnp.bfloat16)
    key_scale = jax.random.uniform(part_keys[1], (BATCH_SIZE, blocks, 1, KV_HEADS, 1), jnp.float32, 0.5, 1.5)
    key_noise = jax.random.normal(part_keys[2], block_shape, jnp.float32) * key_scale
    k_cache = key_noise.reshape(cache_shape) + query_shift(hidden, w_query)[:, None]
    v_base = jax.random.normal(part_keys[3], (BATCH_SIZE, blocks, 1, KV_HEADS, HEAD_DIM), jnp.float32)
    v_cache = (v_base + jax.random.normal(part_keys[4], block_shape, jnp.float32)).reshape(cache_shape)
    positions = jax.random.randint(part_keys[5], (BATCH_SIZE,), SEQ_LEN // 4, SEQ_LEN, dtype=jnp.int32)
    return {'hidden': hidden, 'w_query': w_query, 'w_key': w_key, 'w_value': w_value, 'w_out': w_out, 'k_cache': k_cache.astype(jnp.bfloat16), 'v_cache': v_cache.astype(jnp.bfloat16), 'positions': positions}


def reference(hidden, w_query, w_key, w_value, w_out, k_cache, v_cache, positions):
    group_size = NUM_HEADS // KV_HEADS
    q_flat = jnp.dot(hidden, w_query, preferred_element_type=jnp.float32).astype(jnp.bfloat16)
    key_new = jnp.dot(hidden, w_key, preferred_element_type=jnp.float32).astype(jnp.bfloat16).reshape(BATCH_SIZE, KV_HEADS, HEAD_DIM)
    value_new = jnp.dot(hidden, w_value, preferred_element_type=jnp.float32).astype(jnp.bfloat16).reshape(BATCH_SIZE, KV_HEADS, HEAD_DIM)
    seq_ids = jnp.arange(SEQ_LEN)
    at_pos = (seq_ids[None, :] == positions[:, None])[:, :, None, None]
    k_updated = jnp.where(at_pos, key_new[:, None], k_cache)
    v_updated = jnp.where(at_pos, value_new[:, None], v_cache)
    is_valid = seq_ids[None, :] <= positions[:, None]
    q_heads = q_flat.astype(jnp.float32).reshape(BATCH_SIZE, KV_HEADS, group_size, HEAD_DIM)

    def one_row(row_args):
        q_row, k_row, v_row, valid_row = row_args
        scores = jnp.einsum('kgd,skd->kgs', q_row, k_row.astype(jnp.float32)) * HEAD_DIM ** -0.5
        scores = jnp.where(valid_row[None, None, :], scores, -jnp.inf)
        weights = jax.nn.softmax(scores, axis=-1)
        return jnp.einsum('kgs,skd->kgd', weights, v_row.astype(jnp.float32))

    attended = lax.map(one_row, (q_heads, k_updated, v_updated, is_valid))
    combined = attended.reshape(BATCH_SIZE, NUM_HEADS * HEAD_DIM).astype(jnp.bfloat16)
    result = jnp.dot(combined, w_out, preferred_element_type=jnp.float32).astype(jnp.bfloat16)
    return result, k_updated, v_updated
```

```python
import functools
import math

import jax
import jax.numpy as jnp
from jax import lax
from jax.experimental import pallas as pl
from jax.experimental.pallas import tpu as pltpu
from jax.sharding import PartitionSpec as P

F32 = jnp.float32
BF16 = jnp.bfloat16
MESH = pl.DeviceIdType.MESH
VMEM = pltpu.VMEM
DMA = pltpu.SemaphoreType.DMA


def place(n):
    me = lax.axis_index('seq')
    chips = n // 2
    side = math.isqrt(chips)
    chip, core = me // 2, me % 2
    row, col = chip // side, chip % side

    def far(d):
        return min(d[0], side - d[0]) + min(d[1], side - d[1])

    offsets = [(dy, dx) for dy in range(side) for dx in range(side) if dy or dx]
    offsets.sort(key=far, reverse=True)

    def ahead(d):
        return ((row + d[0]) % side) * side + (col + d[1]) % side

    def behind(d):
        return ((row + side - d[0]) % side) * side + (col + side - d[1]) % side

    return me, chip, core, offsets, ahead, behind


def remote(src, dst, send, recv, device):
    return pltpu.make_async_remote_copy(src_ref=src, dst_ref=dst, send_sem=send, recv_sem=recv,
                                        device_id={'seq': device}, device_id_type=MESH)


def greet(core, chip, offsets, ahead):
    barrier = pltpu.get_barrier_semaphore()
    for d in offsets:
        pl.semaphore_signal(barrier, inc=1, device_id={'seq': ahead(d) * 2 + core}, device_id_type=MESH)
    pl.semaphore_signal(barrier, inc=1, device_id={'seq': chip * 2 + 1 - core}, device_id_type=MESH)
    return barrier


def gather_blocks(block, chip, core, offsets, ahead, behind, sems):
    send, recv, fsend, frecv = sems
    partner = chip * 2 + 1 - core
    started = []
    for d in offsets:
        cp = remote(block(core, chip), block(core, chip), send.at[ahead(d)], recv.at[chip], ahead(d) * 2 + core)
        cp.start()
        started.append(cp)
    cp = remote(block(core, chip), block(core, chip), fsend.at[chip], frecv.at[chip], partner)
    cp.start()
    started.append(cp)
    for d in offsets:
        src = behind(d)
        got = block(core, src)
        remote(got, got, send.at[src], recv.at[src], partner).wait_recv()
        cp = remote(got, got, fsend.at[src], frecv.at[src], partner)
        cp.start()
        started.append(cp)
    for src in [chip] + [behind(d) for d in offsets]:
        got = block(1 - core, src)
        remote(got, got, fsend.at[src], frecv.at[src], partner).wait_recv()
    for cp in started:
        cp.wait_send()


def qkv_kernel(n, x_ref, wq_ref, wk_ref, wv_ref, g_ref, wbuf, wsem, send, recv, fsend, frecv):
    me, chip, core, offsets, ahead, behind = place(n)
    barrier = greet(core, chip, offsets, ahead)
    batch, depth = x_ref.shape
    parts = wsem.shape[1]
    step = depth // parts
    wide = wbuf.shape[1] // 2
    kv_heads = wk_ref.shape[1] // wide

    def fetch(w_ref, block, side, j):
        return pltpu.make_async_copy(
            w_ref.at[pl.ds(j * step, step), pl.ds(pl.multiple_of(block * wide, wide), wide)],
            wbuf.at[pl.ds(j * step, step), pl.ds(side * wide, wide)], wsem.at[side, j])

    for j in range(parts):
        fetch(wq_ref, me, 0, j).start()

        @pl.when(chip < kv_heads)
        def _():
            fetch(wk_ref, chip % kv_heads, 1, j).start()

        @pl.when(chip >= kv_heads)
        def _():
            fetch(wv_ref, chip % kv_heads, 1, j).start()

    acc = None
    for j in range(parts):
        fetch(wq_ref, 0, 0, j).wait()
        fetch(wk_ref, 0, 1, j).wait()
        part = jnp.dot(x_ref[:, j * step:(j + 1) * step], wbuf[j * step:(j + 1) * step, :], preferred_element_type=F32)
        acc = part if acc is None else acc + part
    half = batch // 2
    g_ref[core, chip, :batch, :] = acc[:, :wide].astype(BF16)
    kv = jnp.where(core == 0, acc[:half, wide:], acc[half:, wide:])
    g_ref[core, chip, batch:, :] = kv.astype(BF16)
    pl.semaphore_wait(barrier, len(offsets) + 1)
    gather_blocks(lambda c, p: g_ref.at[c, p], chip, core, offsets, ahead, behind, (send, recv, fsend, frecv))


def attend_kernel(pos_ref, g_ref, k_ref, v_ref, ko_ref, vo_ref, o_ref, kbuf, vbuf, qf, knf, vnf, st, sem):
    chunks, per, length, kv_heads, wide = kbuf.shape
    batch = chunks * per
    rows = qf.shape[0] // batch
    chips = rows // 2
    half = batch // 2
    pitch = o_ref.shape[0] // rows
    base = lax.axis_index('seq') * length

    def k_in(i):
        return pltpu.make_async_copy(k_ref.at[pl.ds(i * per, per)], kbuf.at[i], sem.at[0, i])

    def v_in(i):
        return pltpu.make_async_copy(v_ref.at[pl.ds(i * per, per)], vbuf.at[i], sem.at[1, i])

    def k_out(i):
        return pltpu.make_async_copy(kbuf.at[i], ko_ref.at[pl.ds(i * per, per)], sem.at[2, i])

    def v_out(i):
        return pltpu.make_async_copy(vbuf.at[i], vo_ref.at[pl.ds(i * per, per)], sem.at[3, i])

    @pl.loop(0, chunks)
    def _(i):
        k_in(i).start()
        v_in(i).start()

    for r in range(rows):
        qf[pl.ds(r, batch, stride=rows), :] = g_ref[r // chips, r % chips, :batch, :].astype(F32)
    for h in range(kv_heads):
        for c in range(2):
            at = pl.ds(c * half * kv_heads + h, half, stride=kv_heads)
            knf[at, :] = g_ref[c, h, batch:, :].astype(F32)
            vnf[at, :] = g_ref[c, kv_heads + h, batch:, :].astype(F32)
    st[...] = jnp.zeros_like(st)
    cols = length * kv_heads
    col = lax.broadcasted_iota(jnp.int32, (rows, cols), 1)
    row = lax.broadcasted_iota(jnp.int32, (rows, cols), 0)
    ours = (col % kv_heads) == ((row % chips) * 2 * kv_heads // rows)
    place_of = jnp.where(ours, col // kv_heads, 2 ** 30)
    lane = lax.broadcasted_iota(jnp.int32, st.shape, 1)

    @pl.loop(0, chunks)
    def _(i):
        k_in(i).wait()
        v_in(i).wait()
        stats = st[...]
        for j in range(per):
            b = i * per + j
            last = pos_ref[b] - base
            here = (last >= 0) & (last < length)
            at = jnp.clip(last, 0, length - 1)
            new = pl.ds(pl.multiple_of(b * kv_heads, kv_heads), kv_heads)
            kbuf[i, j, at] = jnp.where(here, knf[new, :], kbuf[i, j, at].astype(F32)).astype(BF16)
            vbuf[i, j, at] = jnp.where(here, vnf[new, :], vbuf[i, j, at].astype(F32)).astype(BF16)
            q = qf[pl.ds(pl.multiple_of(b * rows, rows), rows), :].astype(BF16)
            keys = kbuf[i, j].reshape(cols, wide)
            vals = vbuf[i, j].reshape(cols, wide)
            s = lax.dot_general(q, keys, (((1,), (1,)), ((), ())), preferred_element_type=F32) * wide ** -0.5
            s = jnp.where(place_of <= last, s, -jnp.inf)
            m = jnp.max(s, axis=1, keepdims=True)
            w = jnp.exp(s - jnp.where(m == -jnp.inf, 0.0, m))
            total = jnp.sum(w, axis=1, keepdims=True)
            o_ref[pl.ds(b, rows, stride=pitch), :] = jnp.dot(w.astype(BF16), vals, preferred_element_type=F32)
            stats = jnp.where(lane == b, m, stats)
            stats = jnp.where(lane == b + batch, total, stats)
        st[...] = stats
        k_out(i).start()
        v_out(i).start()

    o_ref[pl.ds(batch, rows, stride=pitch), :] = st[...]

    @pl.loop(0, chunks)
    def _(i):
        k_out(i).wait()
        v_out(i).wait()


def merge_kernel(n, o_ref, wo_ref, y_ref, theirs, mine, got, part, ptheirs, pmine, pgot,
                 xs, xr, s1, r1, s2, r2, send, recv, fsend, frecv):
    me, chip, core, offsets, ahead, behind = place(n)
    chips = n // 2
    partner = chip * 2 + 1 - core
    batch, wide = y_ref.shape[0], wo_ref.shape[0]
    pitch = theirs.shape[0] // chips
    barrier = greet(core, chip, offsets, ahead)
    pl.semaphore_wait(barrier, len(offsets) + 1)

    def lanes(x):
        return pltpu.roll(x, batch, 1)

    swap = remote(o_ref.at[pl.ds((1 - core) * chips * pitch, chips * pitch)], theirs, xs.at[0], xr.at[0], partner)
    swap.start()
    swap.wait_recv()
    first = pl.multiple_of(core * chips * pitch, chips * pitch)
    sa = o_ref[pl.ds(first + batch, chips, stride=pitch), :]
    sb = theirs[pl.ds(batch, chips, stride=pitch), :]
    m = jnp.maximum(sa, sb)
    safe = jnp.where(m == -jnp.inf, 0.0, m)
    wa, wb = jnp.exp(sa - safe), jnp.exp(sb - safe)
    total = lanes(sa) * wa + lanes(sb) * wb
    lane = lax.broadcasted_iota(jnp.int32, m.shape, 1)
    mine[pl.ds(batch, chips, stride=pitch), :] = jnp.where(lane < batch, m, lanes(total))
    wt = jnp.concatenate([wa, wb], axis=0).T
    for p in range(chips):
        a = o_ref[pl.ds(first + p * pitch, batch), :] * wt[:batch, p:p + 1]
        b = theirs[p * pitch:p * pitch + batch, :] * wt[:batch, chips + p:chips + p + 1]
        mine[p * pitch:p * pitch + batch, :] = a + b

    def slot(ref, p):
        size = ref.shape[0] // chips
        return ref.at[pl.ds(pl.multiple_of(p * size, size), size)]

    started = []
    for d in offsets:
        to = ahead(d)
        cp = remote(slot(mine, to), slot(got, chip), s1.at[to], r1.at[chip], to * 2 + core)
        cp.start()
        started.append(cp)
    own = pl.ds(pl.multiple_of(chip * pitch, pitch), pitch)
    got[own, :] = mine[own, :]
    for d in offsets:
        src = behind(d)
        remote(slot(got, src), slot(got, src), s1.at[src], r1.at[src], partner).wait_recv()
    s = got[pl.ds(batch, chips, stride=pitch), :]
    w = jnp.exp(s - jnp.max(s, axis=0, keepdims=True))
    w = w / jnp.sum(lanes(s) * w, axis=0, keepdims=True)
    wt = w.T
    out = got[:batch, :] * wt[:batch, 0:1]
    for p in range(1, chips):
        out = out + got[p * pitch:p * pitch + batch, :] * wt[:batch, p:p + 1]
    out = out.astype(BF16)
    for p in range(chips):
        r = jnp.dot(out, wo_ref[:, p * 2 * wide:(p + 1) * 2 * wide], preferred_element_type=F32)
        part[0, p * batch:(p + 1) * batch, :] = r[:, :wide]
        part[1, p * batch:(p + 1) * batch, :] = r[:, wide:]
    swap2 = remote(part.at[1 - core], ptheirs, xs.at[1], xr.at[1], partner)
    swap2.start()
    swap2.wait_recv()
    pmine[...] = part[core] + ptheirs[...]
    for d in offsets:
        to = ahead(d)
        cp = remote(slot(pmine, to), slot(pgot, chip), s2.at[to], r2.at[chip], to * 2 + core)
        cp.start()
        started.append(cp)
    own = pl.ds(pl.multiple_of(chip * batch, batch), batch)
    pgot[own, :] = pmine[own, :]
    for d in offsets:
        src = behind(d)
        remote(slot(pgot, src), slot(pgot, src), s2.at[src], r2.at[src], partner).wait_recv()
    y = pgot[:batch, :]
    for p in range(1, chips):
        y = y + pgot[p * batch:(p + 1) * batch, :]
    y_ref[:, pl.ds(pl.multiple_of(me * wide, wide), wide)] = y.astype(BF16)

    def block(c, p):
        return y_ref.at[:, pl.ds(pl.multiple_of((p * 2 + c) * wide, wide), wide)]

    gather_blocks(block, chip, core, offsets, ahead, behind, (send, recv, fsend, frecv))
    swap.wait_send()
    swap2.wait_send()
    for cp in started:
        cp.wait_send()


def solution(mesh):
    n = mesh.shape['seq']
    chips = n // 2
    cache_spec = P('rep', 'seq', None, None)
    in_specs = (P('rep', None), P(), P(), P(), P('seq', None), cache_spec, cache_spec, P('rep'))
    out_specs = (P('rep', None), cache_spec, cache_spec)
    vmem = pl.BlockSpec(memory_space=pltpu.VMEM)
    smem = pl.BlockSpec(memory_space=pltpu.SMEM)
    hbm = pl.BlockSpec(memory_space=pl.ANY)

    def step(x, wq, wk, wv, wo, k, v, pos):
        batch, depth = x.shape
        length, kv_heads, wide = k.shape[1:]
        heads = wq.shape[1] // wide
        slots = DMA((chips,))
        g = pl.pallas_call(
            functools.partial(qkv_kernel, n),
            out_shape=jax.ShapeDtypeStruct((2, chips, batch + batch // 2, wide), BF16),
            in_specs=[vmem, hbm, hbm, hbm], out_specs=vmem,
            scratch_shapes=[VMEM((depth, 2 * wide), BF16), DMA((2, 4)), slots, slots, slots, slots],
            compiler_params=pltpu.CompilerParams(collective_id=0, has_side_effects=True),
            name='project',
        )(x, wq, wk, wv)
        per = 4
        pitch = batch + 8
        ko, vo, o = pl.pallas_call(
            attend_kernel,
            out_shape=[jax.ShapeDtypeStruct(k.shape, k.dtype), jax.ShapeDtypeStruct(v.shape, v.dtype),
                       jax.ShapeDtypeStruct((heads * pitch, wide), F32)],
            in_specs=[smem, vmem, hbm, hbm], out_specs=[hbm, hbm, vmem],
            scratch_shapes=[VMEM((batch // per, per, length, kv_heads, wide), BF16)] * 2 + [
                VMEM((batch * heads, wide), F32), VMEM((batch * kv_heads, wide), F32),
                VMEM((batch * kv_heads, wide), F32), VMEM((heads, wide), F32), DMA((4, batch // per))],
            name='attend',
        )(pos, g, k, v)
        y = pl.pallas_call(
            functools.partial(merge_kernel, n),
            out_shape=jax.ShapeDtypeStruct((batch, depth), BF16),
            in_specs=[vmem, vmem], out_specs=vmem,
            scratch_shapes=[VMEM((chips * pitch, wide), F32)] * 3 + [VMEM((2, chips * batch, wide), F32)]
            + [VMEM((chips * batch, wide), F32)] * 3 + [DMA((2,))] * 2 + [slots] * 8,
            compiler_params=pltpu.CompilerParams(collective_id=1, has_side_effects=True),
            name='merge',
        )(o, wo)
        return y, ko, vo

    return jax.shard_map(step, mesh=mesh, in_specs=in_specs, out_specs=out_specs, check_vma=False)
```

```python
import functools
import math

import jax
import jax.numpy as jnp
from jax import lax
from jax.experimental import pallas as pl
from jax.experimental.pallas import tpu as pltpu
from jax.sharding import PartitionSpec as P

F32 = jnp.float32
BF16 = jnp.bfloat16
MESH = pl.DeviceIdType.MESH
VMEM = pltpu.VMEM
DMA = pltpu.SemaphoreType.DMA


def place(n):
    me = lax.axis_index('seq')
    chips = n // 2
    side = math.isqrt(chips)
    chip, core = me // 2, me % 2
    row, col = chip // side, chip % side

    def far(d):
        return min(d[0], side - d[0]) + min(d[1], side - d[1])

    offsets = [(dy, dx) for dy in range(side) for dx in range(side) if dy or dx]
    offsets.sort(key=far, reverse=True)

    def ahead(d):
        return ((row + d[0]) % side) * side + (col + d[1]) % side

    def behind(d):
        return ((row + side - d[0]) % side) * side + (col + side - d[1]) % side

    return me, chip, core, offsets, ahead, behind


def remote(src, dst, send, recv, device):
    return pltpu.make_async_remote_copy(src_ref=src, dst_ref=dst, send_sem=send, recv_sem=recv,
                                        device_id={'seq': device}, device_id_type=MESH)


def greet(core, chip, offsets, ahead):
    barrier = pltpu.get_barrier_semaphore()
    for d in offsets:
        pl.semaphore_signal(barrier, inc=1, device_id={'seq': ahead(d) * 2 + core}, device_id_type=MESH)
    pl.semaphore_signal(barrier, inc=1, device_id={'seq': chip * 2 + 1 - core}, device_id_type=MESH)
    return barrier


def gather_blocks(block, chip, core, offsets, ahead, behind, sems, took=None):
    send, recv, fsend, frecv = sems
    partner = chip * 2 + 1 - core
    started = []
    for d in offsets:
        cp = remote(block(core, chip), block(core, chip), send.at[ahead(d)], recv.at[chip], ahead(d) * 2 + core)
        cp.start()
        started.append(cp)
    cp = remote(block(core, chip), block(core, chip), fsend.at[chip], frecv.at[chip], partner)
    cp.start()
    started.append(cp)
    if took is not None:
        took(core, chip)
    for d in offsets:
        src = behind(d)
        got = block(core, src)
        remote(got, got, send.at[src], recv.at[src], partner).wait_recv()
        cp = remote(got, got, fsend.at[src], frecv.at[src], partner)
        cp.start()
        started.append(cp)
        if took is not None:
            took(core, src)
    for src in [chip] + [behind(d) for d in offsets]:
        got = block(1 - core, src)
        remote(got, got, fsend.at[src], frecv.at[src], partner).wait_recv()
        if took is not None:
            took(1 - core, src)
    return started


def decode_kernel(n, pos_ref, x_ref, wq_ref, wk_ref, wv_ref, wo_ref, k_ref, v_ref, y_ref, kn_ref, vn_ref,
                  wbuf, g_ref, kbuf, vbuf, qf, kvf, st, o_ref, theirs, mine, got, part, ptheirs, pmine, pgot,
                  wsem, ksem, asend, arecv, afsend, afrecv, xs, xr, s1, r1, s2, r2, send, recv, fsend, frecv):
    me, chip, core, offsets, ahead, behind = place(n)
    chips = n // 2
    partner = chip * 2 + 1 - core
    barrier = greet(core, chip, offsets, ahead)
    batch, depth = x_ref.shape
    wide = wbuf.shape[1] // 2
    groups, per, length, kv_heads, _ = kbuf.shape
    rows = qf.shape[0] // batch
    half = batch // 2
    pitch = theirs.shape[0] // chips
    base = me * length

    parts = wsem.shape[1]
    step = depth // parts

    def fetch(w_ref, block, side, j):
        return pltpu.make_async_copy(
            w_ref.at[pl.ds(j * step, step), pl.ds(pl.multiple_of(block * wide, wide), wide)],
            wbuf.at[pl.ds(j * step, step), pl.ds(side * wide, wide)], wsem.at[side, j])

    for j in range(parts):
        fetch(wq_ref, me, 0, j).start()

        @pl.when(chip < kv_heads)
        def _():
            fetch(wk_ref, chip % kv_heads, 1, j).start()

        @pl.when(chip >= kv_heads)
        def _():
            fetch(wv_ref, chip % kv_heads, 1, j).start()

    def k_in(i):
        return pltpu.make_async_copy(k_ref.at[:, i], kbuf.at[i], ksem.at[0, i])

    def v_in(i):
        return pltpu.make_async_copy(v_ref.at[:, i], vbuf.at[i], ksem.at[1, i])

    @pl.loop(0, groups)
    def _(i):
        k_in(i).start()
        v_in(i).start()

    st[...] = jnp.zeros_like(st)
    acc = None
    for j in range(parts):
        fetch(wq_ref, 0, 0, j).wait()
        fetch(wk_ref, 0, 1, j).wait()
        one = jnp.dot(x_ref[:, j * step:(j + 1) * step], wbuf[j * step:(j + 1) * step, :], preferred_element_type=F32)
        acc = one if acc is None else acc + one
    g_ref[core, chip, :batch, :] = acc[:, :wide].astype(BF16)
    kv = jnp.where(core == 0, acc[:half, wide:], acc[half:, wide:])
    g_ref[core, chip, batch:, :] = kv.astype(BF16)
    pl.semaphore_wait(barrier, len(offsets) + 1)

    def took(c, p):
        r = c * chips + p
        for j in range(per):
            qf[pl.ds(j * rows + r, groups, stride=per * rows), :] = g_ref[c, p, j * groups:(j + 1) * groups, :].astype(F32)
        at = (p // kv_heads) * batch * kv_heads + c * half * kv_heads + p % kv_heads
        kvf[pl.ds(at, half, stride=kv_heads), :] = g_ref[c, p, batch:, :].astype(F32)

    started = gather_blocks(lambda c, p: g_ref.at[c, p], chip, core, offsets, ahead, behind,
                            (asend, arecv, afsend, afrecv), took)

    cols = length * kv_heads
    lane = lax.broadcasted_iota(jnp.int32, (kv_heads, wide), 1)
    sub = lax.broadcasted_iota(jnp.int32, (kv_heads, wide), 0)
    ours = sub == ((lane % chips) * 2 * kv_heads // rows)
    quarter = lane // rows
    wlane = lax.broadcasted_iota(jnp.int32, (wide, wide), 1) // rows

    @pl.loop(0, groups)
    def _(i):
        k_in(i).wait()
        v_in(i).wait()
        last = jnp.zeros((kv_heads, wide), jnp.int32)
        for j in range(per):
            b = j * groups + i
            end = pos_ref[b] - base
            last = jnp.where(quarter == j, end, last)
            here = (end >= 0) & (end < length)
            at = jnp.clip(end, 0, length - 1)
            new = kvf[pl.ds(pl.multiple_of(b * kv_heads, kv_heads), kv_heads), :].astype(BF16)
            kn_ref[b] = new
            kbuf[i, j] = jnp.where(patch_rows(length, kv_heads, wide, at, here), new[None], kbuf[i, j])
            new = kvf[pl.ds(pl.multiple_of((batch + b) * kv_heads, kv_heads), kv_heads), :].astype(BF16)
            vn_ref[b] = new
            vbuf[i, j] = jnp.where(patch_rows(length, kv_heads, wide, at, here), new[None], vbuf[i, j])
        limit = jnp.where(ours, last, -1)
        qt = qf[pl.ds(pl.multiple_of(i * per * rows, per * rows), per * rows), :].T.astype(BF16)
        keys = jnp.concatenate([kbuf[i, j].reshape(cols, wide) for j in range(per)], axis=1)
        query = jnp.concatenate([jnp.where(wlane == j, qt, 0) for j in range(per)], axis=0)
        s = jnp.dot(keys, query, preferred_element_type=F32).reshape(length, kv_heads, wide) * wide ** -0.5
        t = lax.broadcasted_iota(jnp.int32, (length, kv_heads, wide), 0)
        s = jnp.where(t <= limit[None], s, -jnp.inf)
        m = jnp.max(jnp.max(s, axis=0), axis=0, keepdims=True)
        w = jnp.exp(s - jnp.where(m == -jnp.inf, 0.0, m)[None])
        st[pl.ds(i, 1), :] = m
        st[pl.ds(groups + i, 1), :] = jnp.sum(jnp.sum(w, axis=0), axis=0, keepdims=True)
        wt = w.reshape(cols, wide).T.astype(BF16)
        for j in range(per):
            o_ref[pl.ds(j * groups + i, rows, stride=pitch), :] = jnp.dot(
                wt[j * rows:(j + 1) * rows, :], vbuf[i, j].reshape(cols, wide), preferred_element_type=F32)

    zt = st[...].T
    slane = lax.broadcasted_iota(jnp.int32, (rows, wide), 1) // groups
    stats = jnp.zeros((rows, wide), F32)
    for j in range(per):
        z = zt[j * rows:(j + 1) * rows, :]
        stats = jnp.where(slane == j, pltpu.roll(z, j * groups, 1) if j else z, stats)
        stats = jnp.where(slane == per + j, pltpu.roll(z, batch + j * groups - groups, 1), stats)
    o_ref[pl.ds(batch, rows, stride=pitch), :] = stats

    def lanes(x):
        return pltpu.roll(x, batch, 1)

    swap = remote(o_ref.at[pl.ds((1 - core) * chips * pitch, chips * pitch)], theirs, xs.at[0], xr.at[0], partner)
    swap.start()
    swap.wait_recv()
    first = pl.multiple_of(core * chips * pitch, chips * pitch)
    sa = o_ref[pl.ds(first + batch, chips, stride=pitch), :]
    sb = theirs[pl.ds(batch, chips, stride=pitch), :]
    m = jnp.maximum(sa, sb)
    safe = jnp.where(m == -jnp.inf, 0.0, m)
    wa, wb = jnp.exp(sa - safe), jnp.exp(sb - safe)
    total = lanes(sa) * wa + lanes(sb) * wb
    lane = lax.broadcasted_iota(jnp.int32, m.shape, 1)
    mine[pl.ds(batch, chips, stride=pitch), :] = jnp.where(lane < batch, m, lanes(total))
    wt = jnp.concatenate([wa, wb], axis=0).T
    for p in range(chips):
        a = o_ref[pl.ds(first + p * pitch, batch), :] * wt[:batch, p:p + 1]
        b = theirs[p * pitch:p * pitch + batch, :] * wt[:batch, chips + p:chips + p + 1]
        mine[p * pitch:p * pitch + batch, :] = a + b

    def slot(ref, p):
        size = ref.shape[0] // chips
        return ref.at[pl.ds(pl.multiple_of(p * size, size), size)]

    for d in offsets:
        to = ahead(d)
        cp = remote(slot(mine, to), slot(got, chip), s1.at[to], r1.at[chip], to * 2 + core)
        cp.start()
        started.append(cp)
    own = pl.ds(pl.multiple_of(chip * pitch, pitch), pitch)
    got[own, :] = mine[own, :]
    for d in offsets:
        src = behind(d)
        remote(slot(got, src), slot(got, src), s1.at[src], r1.at[src], partner).wait_recv()
    s = got[pl.ds(batch, chips, stride=pitch), :]
    w = jnp.exp(s - jnp.max(s, axis=0, keepdims=True))
    w = w / jnp.sum(lanes(s) * w, axis=0, keepdims=True)
    wt = w.T
    out = got[:batch, :] * wt[:batch, 0:1]
    for p in range(1, chips):
        out = out + got[p * pitch:p * pitch + batch, :] * wt[:batch, p:p + 1]
    out = out.astype(BF16)
    for p in range(chips):
        r = jnp.dot(out, wo_ref[:, p * 2 * wide:(p + 1) * 2 * wide], preferred_element_type=F32)
        part[0, p * batch:(p + 1) * batch, :] = r[:, :wide]
        part[1, p * batch:(p + 1) * batch, :] = r[:, wide:]
    swap2 = remote(part.at[1 - core], ptheirs, xs.at[1], xr.at[1], partner)
    swap2.start()
    swap2.wait_recv()
    pmine[...] = part[core] + ptheirs[...]
    for d in offsets:
        to = ahead(d)
        cp = remote(slot(pmine, to), slot(pgot, chip), s2.at[to], r2.at[chip], to * 2 + core)
        cp.start()
        started.append(cp)
    own = pl.ds(pl.multiple_of(chip * batch, batch), batch)
    pgot[own, :] = pmine[own, :]
    for d in offsets:
        src = behind(d)
        remote(slot(pgot, src), slot(pgot, src), s2.at[src], r2.at[src], partner).wait_recv()
    y = pgot[:batch, :]
    for p in range(1, chips):
        y = y + pgot[p * batch:(p + 1) * batch, :]
    y_ref[:, pl.ds(pl.multiple_of(me * wide, wide), wide)] = y.astype(BF16)

    def block(c, p):
        return y_ref.at[:, pl.ds(pl.multiple_of((p * 2 + c) * wide, wide), wide)]

    started += gather_blocks(block, chip, core, offsets, ahead, behind, (send, recv, fsend, frecv))
    swap.wait_send()
    swap2.wait_send()
    for cp in started:
        cp.wait_send()


def store_kernel(pos_ref, k_ref, v_ref, kn_ref, vn_ref, y_ref, ko_ref, vo_ref, yo_ref, sem, rsem, ysem):
    batch, length = k_ref.shape[:2]
    chunks = sem.shape[1]
    per = batch // chunks
    base = lax.axis_index('seq') * length

    def whole(src, dst, a, i):
        return pltpu.make_async_copy(src.at[pl.ds(i * per, per)], dst.at[pl.ds(i * per, per)], sem.at[a, i])

    def row(src, dst, a, b):
        at = jnp.clip(pos_ref[b] - base, 0, length - 1)
        return pltpu.make_async_copy(src.at[b], dst.at[b, at], rsem.at[a, b])

    def here(b):
        end = pos_ref[b] - base
        return (end >= 0) & (end < length)

    @pl.loop(0, chunks)
    def _(i):
        whole(k_ref, ko_ref, 0, i).start()
        whole(v_ref, vo_ref, 1, i).start()

    y = pltpu.make_async_copy(y_ref, yo_ref, ysem)
    y.start()

    @pl.loop(0, chunks)
    def _(i):
        whole(k_ref, ko_ref, 0, i).wait()
        whole(v_ref, vo_ref, 1, i).wait()
        for j in range(per):
            b = i * per + j

            @pl.when(here(b))
            def _():
                row(kn_ref, ko_ref, 0, b).start()
                row(vn_ref, vo_ref, 1, b).start()

    y.wait()

    @pl.loop(0, batch)
    def _(b):
        @pl.when(here(b))
        def _():
            row(kn_ref, ko_ref, 0, b).wait()
            row(vn_ref, vo_ref, 1, b).wait()


def patch_rows(length, kv_heads, wide, at, here):
    t = lax.broadcasted_iota(jnp.int32, (length, kv_heads, wide), 0)
    return (t == at) & here


def solution(mesh):
    n = mesh.shape['seq']
    chips = n // 2
    cache_spec = P('rep', 'seq', None, None)
    in_specs = (P('rep', None), P(), P(), P(), P('seq', None), cache_spec, cache_spec, P('rep'))
    out_specs = (P('rep', None), cache_spec, cache_spec)
    vmem = pl.BlockSpec(memory_space=pltpu.VMEM)
    smem = pl.BlockSpec(memory_space=pltpu.SMEM)
    hbm = pl.BlockSpec(memory_space=pltpu.HBM)
    anywhere = pl.BlockSpec(memory_space=pl.ANY)

    def step(x, wq, wk, wv, wo, k, v, pos):
        batch, depth = x.shape
        length, kv_heads, wide = k.shape[1:]
        heads = wq.shape[1] // wide
        slots = DMA((chips,))
        per = wide // heads
        groups = batch // per
        pitch = batch + 8
        split = (per, groups, length, kv_heads, wide)
        cache = VMEM((groups, per, length, kv_heads, wide), BF16)
        new = jax.ShapeDtypeStruct((batch, kv_heads, wide), BF16)
        y, kn, vn = pl.pallas_call(
            functools.partial(decode_kernel, n),
            out_shape=[jax.ShapeDtypeStruct((batch, depth), BF16), new, new],
            in_specs=[smem, vmem, hbm, hbm, hbm, vmem, hbm, hbm], out_specs=[vmem] * 3,
            scratch_shapes=[
                VMEM((depth, 2 * wide), BF16), VMEM((2, chips, batch + batch // 2, wide), BF16), cache, cache,
                VMEM((batch * heads, wide), F32), VMEM((2 * batch * kv_heads, wide), F32), VMEM((wide, wide), F32),
                VMEM((heads * pitch, wide), F32)]
            + [VMEM((chips * pitch, wide), F32)] * 3 + [VMEM((2, chips * batch, wide), F32)]
            + [VMEM((chips * batch, wide), F32)] * 3 + [DMA((2, 4)), DMA((2, groups))] + [slots] * 4
            + [DMA((2,))] * 2 + [slots] * 8,
            compiler_params=pltpu.CompilerParams(collective_id=0, has_side_effects=True, vmem_limit_bytes=44 << 20),
            cost_estimate=pl.CostEstimate(flops=10 ** 10, bytes_accessed=32 << 20, transcendentals=0),
            name='decode',
        )(pos, x, wq, wk, wv, wo, k.reshape(split), v.reshape(split))
        chunks = 16
        ko, vo, y = pl.pallas_call(
            store_kernel,
            out_shape=[jax.ShapeDtypeStruct(k.shape, k.dtype), jax.ShapeDtypeStruct(v.shape, v.dtype),
                       jax.ShapeDtypeStruct((batch, depth), BF16)],
            in_specs=[smem, anywhere, anywhere, vmem, vmem, vmem], out_specs=[hbm, hbm, hbm],
            scratch_shapes=[DMA((2, chunks)), DMA((2, batch)), DMA],
            compiler_params=pltpu.CompilerParams(vmem_limit_bytes=4 << 20),
            cost_estimate=pl.CostEstimate(flops=10 ** 8, bytes_accessed=32 << 20, transcendentals=0),
            name='store',
        )(pos, k, v, kn, vn, y)
        return y, ko, vo

    return jax.shard_map(step, mesh=mesh, in_specs=in_specs, out_specs=out_specs, check_vma=False)
```

```python
import functools
import math

import jax
import jax.numpy as jnp
from jax import lax
from jax.experimental import pallas as pl
from jax.experimental.pallas import tpu as pltpu
from jax.sharding import PartitionSpec as P

F32 = jnp.float32
BF16 = jnp.bfloat16
MESH = pl.DeviceIdType.MESH
VMEM = pltpu.VMEM
DMA = pltpu.SemaphoreType.DMA


def place(n):
    me = lax.axis_index('seq')
    chips = n // 2
    side = math.isqrt(chips)
    chip, core = me // 2, me % 2
    row, col = chip // side, chip % side

    def far(d):
        return min(d[0], side - d[0]) + min(d[1], side - d[1])

    offsets = [(dy, dx) for dy in range(side) for dx in range(side) if dy or dx]
    offsets.sort(key=far, reverse=True)

    def ahead(d):
        return ((row + d[0]) % side) * side + (col + d[1]) % side

    def behind(d):
        return ((row + side - d[0]) % side) * side + (col + side - d[1]) % side

    return me, chip, core, offsets, ahead, behind


def remote(src, dst, send, recv, device):
    return pltpu.make_async_remote_copy(src_ref=src, dst_ref=dst, send_sem=send, recv_sem=recv,
                                        device_id={'seq': device}, device_id_type=MESH)


def greet(core, chip, offsets, ahead):
    barrier = pltpu.get_barrier_semaphore()
    for d in offsets:
        pl.semaphore_signal(barrier, inc=1, device_id={'seq': ahead(d) * 2 + core}, device_id_type=MESH)
    pl.semaphore_signal(barrier, inc=1, device_id={'seq': chip * 2 + 1 - core}, device_id_type=MESH)
    return barrier


def gather_blocks(block, chip, core, offsets, ahead, behind, sems, took=None):
    send, recv, fsend, frecv = sems
    partner = chip * 2 + 1 - core
    started = []
    for d in offsets:
        cp = remote(block(core, chip), block(core, chip), send.at[ahead(d)], recv.at[chip], ahead(d) * 2 + core)
        cp.start()
        started.append(cp)
    cp = remote(block(core, chip), block(core, chip), fsend.at[chip], frecv.at[chip], partner)
    cp.start()
    started.append(cp)
    if took is not None:
        took(core, chip)
    for d in offsets:
        src = behind(d)
        got = block(core, src)
        remote(got, got, send.at[src], recv.at[src], partner).wait_recv()
        cp = remote(got, got, fsend.at[src], frecv.at[src], partner)
        cp.start()
        started.append(cp)
        if took is not None:
            took(core, src)
    for src in [chip] + [behind(d) for d in offsets]:
        got = block(1 - core, src)
        remote(got, got, fsend.at[src], frecv.at[src], partner).wait_recv()
        if took is not None:
            took(1 - core, src)
    return started


def decode_kernel(n, pos_ref, x_ref, wq_ref, wk_ref, wv_ref, wo_ref, k_ref, v_ref, y_ref, kn_ref, vn_ref,
                  pos, x, wo, wbuf, g_ref, kbuf, vbuf, qf, kvf, o_ref, theirs, mine, got, part, ptheirs, pmine, pgot,
                  isem, wsem, ksem, asend, arecv, afsend, afrecv, xs, xr, s1, r1, s2, r2, send, recv, fsend, frecv):
    me, chip, core, offsets, ahead, behind = place(n)
    chips = n // 2
    partner = chip * 2 + 1 - core
    barrier = greet(core, chip, offsets, ahead)
    batch, depth = x.shape
    wide = wbuf.shape[1] // 2
    groups, per, length, kv_heads, _ = kbuf.shape
    rows = qf.shape[0] // batch
    half = batch // 2
    halves = theirs.shape[0]
    pitch = theirs.shape[1] // chips
    share = batch // halves
    base = me * length

    parts = wsem.shape[1]
    step = depth // parts

    def fetch(w_ref, block, side, j):
        return pltpu.make_async_copy(
            w_ref.at[pl.ds(j * step, step), pl.ds(pl.multiple_of(block * wide, wide), wide)],
            wbuf.at[pl.ds(j * step, step), pl.ds(side * wide, wide)], wsem.at[side, j])

    get_x = pltpu.make_async_copy(x_ref, x, isem.at[0])
    get_x.start()
    for j in range(parts):
        fetch(wq_ref, me, 0, j).start()

        @pl.when(chip < kv_heads)
        def _():
            fetch(wk_ref, chip % kv_heads, 1, j).start()

        @pl.when(chip >= kv_heads)
        def _():
            fetch(wv_ref, chip % kv_heads, 1, j).start()

    get_pos = pltpu.make_async_copy(pos_ref, pos, isem.at[1])
    get_pos.start()

    def k_in(i):
        return pltpu.make_async_copy(k_ref.at[pl.ds(i * per, per)], kbuf.at[i], ksem.at[0, i])

    def v_in(i):
        return pltpu.make_async_copy(v_ref.at[pl.ds(i * per, per)], vbuf.at[i], ksem.at[1, i])

    get_x.wait()
    acc = None
    for j in range(parts):
        fetch(wq_ref, 0, 0, j).wait()
        fetch(wk_ref, 0, 1, j).wait()
        one = jnp.dot(x[:, j * step:(j + 1) * step], wbuf[j * step:(j + 1) * step, :], preferred_element_type=F32)
        acc = one if acc is None else acc + one
    g_ref[core, chip, :batch, :] = acc[:, :wide].astype(BF16)
    kv = jnp.where(core == 0, acc[:half, wide:], acc[half:, wide:])
    g_ref[core, chip, batch:, :] = kv.astype(BF16)

    @pl.loop(0, groups)
    def _(i):
        k_in(i).start()
        v_in(i).start()

    get_wo = pltpu.make_async_copy(wo_ref, wo, isem.at[2])
    get_wo.start()
    pl.semaphore_wait(barrier, len(offsets) + 1)

    def took(c, p):
        qf[pl.ds(c * chips + p, batch, stride=rows), :] = g_ref[c, p, :batch, :].astype(F32)
        at = (p // kv_heads) * batch * kv_heads + c * half * kv_heads + p % kv_heads
        kvf[pl.ds(at, half, stride=kv_heads), :] = g_ref[c, p, batch:, :].astype(F32)

    started = gather_blocks(lambda c, p: g_ref.at[c, p], chip, core, offsets, ahead, behind,
                            (asend, arecv, afsend, afrecv), took)
    get_pos.wait()

    cols = length * kv_heads
    lanes = per * rows
    lane = lax.broadcasted_iota(jnp.int32, (kv_heads, lanes), 1)
    sub = lax.broadcasted_iota(jnp.int32, (kv_heads, lanes), 0)
    ours = sub == ((lane % chips) * 2 * kv_heads // rows)
    member = lane // rows
    qlane = lax.broadcasted_iota(jnp.int32, (wide, lanes), 1) // rows
    slane = lax.broadcasted_iota(jnp.int32, (rows, wide), 1)

    def attend(i, stats):
        k_in(i).wait()
        v_in(i).wait()
        end = jnp.zeros((kv_heads, lanes), jnp.int32)
        fresh = []
        for j in range(per):
            b = i * per + j
            end = jnp.where(member == j, pos[b] - base, end)
            kn = kvf[pl.ds(pl.multiple_of(b * kv_heads, kv_heads), kv_heads), :].astype(BF16)
            vn = kvf[pl.ds(pl.multiple_of((batch + b) * kv_heads, kv_heads), kv_heads), :].astype(BF16)
            kn_ref[b] = kn
            vn_ref[b] = vn
            fresh.append((kn, vn))
        qt = qf[pl.ds(pl.multiple_of(i * lanes, lanes), lanes), :].T.astype(BF16)
        query = jnp.concatenate([jnp.where(qlane == j, qt, 0) for j in range(per)], axis=0)
        keys = jnp.concatenate([kbuf[i, j].reshape(cols, wide) for j in range(per)], axis=1)
        scale = wide ** -0.5
        s = jnp.dot(keys, query, preferred_element_type=F32).reshape(length, kv_heads, lanes) * scale
        newest = jnp.dot(jnp.concatenate([f[0] for f in fresh], axis=1), query, preferred_element_type=F32) * scale
        t = lax.broadcasted_iota(jnp.int32, (length, kv_heads, lanes), 0)
        s = jnp.where(t < jnp.where(ours, end, 0)[None], s, -jnp.inf)
        newest = jnp.where(ours & (end >= 0) & (end < length), newest, -jnp.inf)
        m = jnp.max(jnp.maximum(jnp.max(s, axis=0), newest), axis=0, keepdims=True)
        safe = jnp.where(m == -jnp.inf, 0.0, m)
        w = jnp.exp(s - safe[None])
        nw = jnp.exp(newest - safe)
        total = jnp.sum(jnp.sum(w, axis=0) + nw, axis=0, keepdims=True)
        wt = w.reshape(cols, lanes).T.astype(BF16)
        extra = jnp.concatenate([nw, m, total, jnp.zeros((kv_heads - 2, lanes), F32)], axis=0).T
        at = (i // (groups // halves)) * rows * pitch + (i % (groups // halves)) * per
        for j in range(0, per, 2):
            both = slice(j * rows, (j + 2) * rows)
            vals = jnp.concatenate([vbuf[i, j].reshape(cols, wide), vbuf[i, j + 1].reshape(cols, wide)], axis=1)
            news = jnp.concatenate([fresh[j][1], fresh[j + 1][1]], axis=1)
            o = jnp.dot(wt[both], vals, preferred_element_type=F32)
            o = o + jnp.dot(extra[both, :kv_heads].astype(BF16), news, preferred_element_type=F32)
            o_ref[pl.ds(at + j, rows, stride=pitch), :] = o[:rows, :wide]
            o_ref[pl.ds(at + j + 1, rows, stride=pitch), :] = o[rows:, wide:]
        for j in range(per):
            z = extra[j * rows:(j + 1) * rows, :]
            stats = jnp.where(slane == i * per + j, z[:, kv_heads:kv_heads + 1], stats)
            stats = jnp.where(slane == batch + i * per + j, z[:, kv_heads + 1:kv_heads + 2], stats)
        return stats

    def other(v):
        return pltpu.roll(v, batch, 1)

    def swap(t):
        return remote(o_ref.at[pl.ds(pl.multiple_of((t * 2 + 1 - core) * chips * pitch, chips * pitch), chips * pitch)],
                      theirs.at[t], xs.at[t], xr.at[t], partner)

    mlane = lax.broadcasted_iota(jnp.int32, (chips, wide), 1)

    def merge_pair(t):
        swap(t).wait_recv()
        first = pl.multiple_of((t * 2 + core) * chips * pitch, chips * pitch)
        sa = o_ref[pl.ds(first + share, chips, stride=pitch), :]
        sb = theirs[t, pl.ds(share, chips, stride=pitch), :]
        m = jnp.maximum(sa, sb)
        safe = jnp.where(m == -jnp.inf, 0.0, m)
        wa, wb = jnp.exp(sa - safe), jnp.exp(sb - safe)
        total = other(sa) * wa + other(sb) * wb
        mine[t, pl.ds(share, chips, stride=pitch), :] = jnp.where(mlane < batch, m, other(total))
        wt = jnp.concatenate([wa, wb], axis=0).T
        mid = slice(t * share, (t + 1) * share)
        for p in range(chips):
            a = o_ref[pl.ds(first + p * pitch, share), :] * wt[mid, p:p + 1]
            b = theirs[t, p * pitch:p * pitch + share, :] * wt[mid, chips + p:chips + p + 1]
            mine[t, p * pitch:p * pitch + share, :] = a + b
        for d in offsets:
            to = ahead(d)
            cp = remote(slot(mine.at[t], to), slot(got.at[t], chip), s1.at[t, to], r1.at[t, chip], to * 2 + core)
            cp.start()
            started.append(cp)
        own = pl.ds(pl.multiple_of(chip * pitch, pitch), pitch)
        got[t, own, :] = mine[t, own, :]

    def slot(ref, p):
        size = ref.shape[0] // chips
        return ref.at[pl.ds(pl.multiple_of(p * size, size), size)]

    def merge_chips(t):
        for d in offsets:
            src = behind(d)
            remote(slot(got.at[t], src), slot(got.at[t], src), s1.at[t, src], r1.at[t, src], partner).wait_recv()
        s = got[t, pl.ds(share, chips, stride=pitch), :]
        w = jnp.exp(s - jnp.max(s, axis=0, keepdims=True))
        w = w / jnp.sum(other(s) * w, axis=0, keepdims=True)
        wt = w.T
        mid = slice(t * share, (t + 1) * share)
        out = got[t, :share, :] * wt[mid, 0:1]
        for p in range(1, chips):
            out = out + got[t, p * pitch:p * pitch + share, :] * wt[mid, p:p + 1]
        return out.astype(BF16)

    each = groups // halves
    for t in range(halves):
        stats = jnp.zeros((rows, wide), F32)
        early = each // 2 if t else 0
        if t:
            stats = lax.fori_loop(t * each, t * each + early, attend, stats)
            merge_pair(t - 1)
        stats = lax.fori_loop(t * each + early, (t + 1) * each, attend, stats)
        o_ref[pl.ds(t * rows * pitch + share, rows, stride=pitch), :] = stats
        swap(t).start()
    merge_pair(halves - 1)
    out = jnp.concatenate([merge_chips(t) for t in range(halves)], axis=0)
    get_wo.wait()
    for p in range(chips):
        r = jnp.dot(out, wo[:, p * 2 * wide:(p + 1) * 2 * wide], preferred_element_type=F32)
        part[0, p * batch:(p + 1) * batch, :] = r[:, :wide]
        part[1, p * batch:(p + 1) * batch, :] = r[:, wide:]
    swap2 = remote(part.at[1 - core], ptheirs, xs.at[halves], xr.at[halves], partner)
    swap2.start()
    swap2.wait_recv()
    pmine[...] = part[core] + ptheirs[...]
    for d in offsets:
        to = ahead(d)
        cp = remote(slot(pmine, to), slot(pgot, chip), s2.at[to], r2.at[chip], to * 2 + core)
        cp.start()
        started.append(cp)
    own = pl.ds(pl.multiple_of(chip * batch, batch), batch)
    pgot[own, :] = pmine[own, :]
    for d in offsets:
        src = behind(d)
        remote(slot(pgot, src), slot(pgot, src), s2.at[src], r2.at[src], partner).wait_recv()
    y = pgot[:batch, :]
    for p in range(1, chips):
        y = y + pgot[p * batch:(p + 1) * batch, :]
    y_ref[:, pl.ds(pl.multiple_of(me * wide, wide), wide)] = y.astype(BF16)

    def block(c, p):
        return y_ref.at[:, pl.ds(pl.multiple_of((p * 2 + c) * wide, wide), wide)]

    started += gather_blocks(block, chip, core, offsets, ahead, behind, (send, recv, fsend, frecv))
    for t in range(halves):
        swap(t).wait_send()
    swap2.wait_send()
    for cp in started:
        cp.wait_send()


def store_kernel(pos_ref, k_ref, v_ref, kn_ref, vn_ref, y_ref, ko_ref, vo_ref, yo_ref, sem, rsem, ysem):
    batch, length = k_ref.shape[:2]
    chunks = sem.shape[1]
    per = batch // chunks
    base = lax.axis_index('seq') * length

    def whole(src, dst, a, i):
        return pltpu.make_async_copy(src.at[pl.ds(i * per, per)], dst.at[pl.ds(i * per, per)], sem.at[a, i])

    def row(src, dst, a, b):
        at = jnp.clip(pos_ref[b] - base, 0, length - 1)
        return pltpu.make_async_copy(src.at[b], dst.at[b, at], rsem.at[a, b])

    def here(b):
        end = pos_ref[b] - base
        return (end >= 0) & (end < length)

    @pl.loop(0, chunks)
    def _(i):
        whole(k_ref, ko_ref, 0, i).start()
        whole(v_ref, vo_ref, 1, i).start()

    y = pltpu.make_async_copy(y_ref, yo_ref, ysem)
    y.start()

    @pl.loop(0, chunks)
    def _(i):
        whole(k_ref, ko_ref, 0, i).wait()
        whole(v_ref, vo_ref, 1, i).wait()
        for j in range(per):
            b = i * per + j

            @pl.when(here(b))
            def _():
                row(kn_ref, ko_ref, 0, b).start()
                row(vn_ref, vo_ref, 1, b).start()

    y.wait()

    @pl.loop(0, batch)
    def _(b):
        @pl.when(here(b))
        def _():
            row(kn_ref, ko_ref, 0, b).wait()
            row(vn_ref, vo_ref, 1, b).wait()


def solution(mesh):
    n = mesh.shape['seq']
    chips = n // 2
    cache_spec = P('rep', 'seq', None, None)
    in_specs = (P('rep', None), P(), P(), P(), P('seq', None), cache_spec, cache_spec, P('rep'))
    out_specs = (P('rep', None), cache_spec, cache_spec)
    vmem = pl.BlockSpec(memory_space=pltpu.VMEM)
    smem = pl.BlockSpec(memory_space=pltpu.SMEM)
    hbm = pl.BlockSpec(memory_space=pltpu.HBM)
    anywhere = pl.BlockSpec(memory_space=pl.ANY)

    def step(x, wq, wk, wv, wo, k, v, pos):
        batch, depth = x.shape
        length, kv_heads, wide = k.shape[1:]
        heads = wq.shape[1] // wide
        slots = DMA((chips,))
        per = 2 * wide // heads
        groups = batch // per
        halves = 2
        pitch = batch // halves + 8
        cache = VMEM((groups, per, length, kv_heads, wide), BF16)
        new = jax.ShapeDtypeStruct((batch, kv_heads, wide), BF16)
        y, kn, vn = pl.pallas_call(
            functools.partial(decode_kernel, n),
            out_shape=[jax.ShapeDtypeStruct((batch, depth), BF16), new, new],
            in_specs=[anywhere] * 8, out_specs=[vmem] * 3,
            scratch_shapes=[
                pltpu.SMEM((batch,), jnp.int32), VMEM((batch, depth), BF16), VMEM(wo.shape, BF16),
                VMEM((depth, 2 * wide), BF16), VMEM((2, chips, batch + batch // 2, wide), BF16), cache, cache,
                VMEM((batch * heads, wide), F32), VMEM((2 * batch * kv_heads, wide), F32),
                VMEM((halves * heads * pitch, wide), F32)]
            + [VMEM((halves, chips * pitch, wide), F32)] * 3 + [VMEM((2, chips * batch, wide), F32)]
            + [VMEM((chips * batch, wide), F32)] * 3 + [DMA((3,)), DMA((2, 4)), DMA((2, groups))] + [slots] * 4
            + [DMA((halves + 1,))] * 2 + [DMA((halves, chips))] * 2 + [slots] * 6,
            compiler_params=pltpu.CompilerParams(collective_id=0, has_side_effects=True, vmem_limit_bytes=45 << 20),
            cost_estimate=pl.CostEstimate(flops=10 ** 10, bytes_accessed=32 << 20, transcendentals=0),
            name='decode',
        )(*(pltpu.with_memory_space_constraint(a, pltpu.HBM) for a in (pos, x, wq, wk, wv, wo, k, v)))
        chunks = 16
        ko, vo, y = pl.pallas_call(
            store_kernel,
            out_shape=[jax.ShapeDtypeStruct(k.shape, k.dtype), jax.ShapeDtypeStruct(v.shape, v.dtype),
                       jax.ShapeDtypeStruct((batch, depth), BF16)],
            in_specs=[smem, anywhere, anywhere, vmem, vmem, vmem], out_specs=[hbm, hbm, hbm],
            scratch_shapes=[DMA((2, chunks)), DMA((2, batch)), DMA],
            compiler_params=pltpu.CompilerParams(vmem_limit_bytes=4 << 20),
            cost_estimate=pl.CostEstimate(flops=10 ** 8, bytes_accessed=32 << 20, transcendentals=0),
            name='store',
        )(pos, k, v, kn, vn, y)
        return y, ko, vo

    return jax.shard_map(step, mesh=mesh, in_specs=in_specs, out_specs=out_specs, check_vma=False)
```

```python
import functools
import math

import jax
import jax.numpy as jnp
from jax import lax
from jax.experimental import pallas as pl
from jax.experimental.pallas import tpu as pltpu
from jax.sharding import PartitionSpec as P

F32 = jnp.float32
BF16 = jnp.bfloat16
MESH = pl.DeviceIdType.MESH
VMEM = pltpu.VMEM
DMA = pltpu.SemaphoreType.DMA


def place(n):
    me = lax.axis_index('seq')
    chips = n // 2
    side = math.isqrt(chips)
    chip, core = me // 2, me % 2
    row, col = chip // side, chip % side

    def far(d):
        return min(d[0], side - d[0]) + min(d[1], side - d[1])

    offsets = [(dy, dx) for dy in range(side) for dx in range(side) if dy or dx]
    offsets.sort(key=far, reverse=True)

    def ahead(d):
        return ((row + d[0]) % side) * side + (col + d[1]) % side

    def behind(d):
        return ((row + side - d[0]) % side) * side + (col + side - d[1]) % side

    return me, chip, core, offsets, ahead, behind


def remote(src, dst, send, recv, device):
    return pltpu.make_async_remote_copy(src_ref=src, dst_ref=dst, send_sem=send, recv_sem=recv,
                                        device_id={'seq': device}, device_id_type=MESH)


def greet(core, chip, offsets, ahead):
    barrier = pltpu.get_barrier_semaphore()
    for d in offsets:
        pl.semaphore_signal(barrier, inc=1, device_id={'seq': ahead(d) * 2 + core}, device_id_type=MESH)
    pl.semaphore_signal(barrier, inc=1, device_id={'seq': chip * 2 + 1 - core}, device_id_type=MESH)
    return barrier


def gather_blocks(block, chip, core, offsets, ahead, behind, sems, took=None):
    send, recv, fsend, frecv = sems
    partner = chip * 2 + 1 - core
    started = []
    for d in offsets:
        cp = remote(block(core, chip), block(core, chip), send.at[ahead(d)], recv.at[chip], ahead(d) * 2 + core)
        cp.start()
        started.append(cp)
    cp = remote(block(core, chip), block(core, chip), fsend.at[chip], frecv.at[chip], partner)
    cp.start()
    started.append(cp)
    if took is not None:
        took(core, chip)
    for d in offsets:
        src = behind(d)
        got = block(core, src)
        remote(got, got, send.at[src], recv.at[src], partner).wait_recv()
        cp = remote(got, got, fsend.at[src], frecv.at[src], partner)
        cp.start()
        started.append(cp)
        if took is not None:
            took(core, src)
    for src in [chip] + [behind(d) for d in offsets]:
        got = block(1 - core, src)
        remote(got, got, fsend.at[src], frecv.at[src], partner).wait_recv()
        if took is not None:
            took(1 - core, src)
    return started


def decode_kernel(n, pos_ref, x_ref, wq_ref, wk_ref, wv_ref, wo_ref, k_ref, v_ref, y_ref, kn_ref, vn_ref,
                  pos, x, wo, wbuf, g_ref, kbuf, vbuf, qf, kvf, raw, wts, mls, o_ref, theirs, mine, got, part, ptheirs, pmine, pgot,
                  isem, wsem, ksem, asend, arecv, afsend, afrecv, xs, xr, s1, r1, s2, r2, send, recv, fsend, frecv):
    me, chip, core, offsets, ahead, behind = place(n)
    chips = n // 2
    partner = chip * 2 + 1 - core
    barrier = greet(core, chip, offsets, ahead)
    batch, depth = x.shape
    wide = wbuf.shape[1] // 2
    groups, per, length, kv_heads, _ = kbuf.shape
    rows = qf.shape[0] // batch
    half = batch // 2
    halves = theirs.shape[0]
    pitch = theirs.shape[1] // chips
    share = batch // halves
    base = me * length

    parts = wsem.shape[1]
    step = depth // parts

    def fetch(w_ref, block, side, j):
        return pltpu.make_async_copy(
            w_ref.at[pl.ds(j * step, step), pl.ds(pl.multiple_of(block * wide, wide), wide)],
            wbuf.at[pl.ds(j * step, step), pl.ds(side * wide, wide)], wsem.at[side, j])

    get_x = pltpu.make_async_copy(x_ref, x, isem.at[0])
    get_x.start()
    for j in range(parts):
        fetch(wq_ref, me, 0, j).start()

        @pl.when(chip < kv_heads)
        def _():
            fetch(wk_ref, chip % kv_heads, 1, j).start()

        @pl.when(chip >= kv_heads)
        def _():
            fetch(wv_ref, chip % kv_heads, 1, j).start()

    get_pos = pltpu.make_async_copy(pos_ref, pos, isem.at[1])
    get_pos.start()

    def k_in(i):
        return pltpu.make_async_copy(k_ref.at[pl.ds(i * per, per)], kbuf.at[i], ksem.at[0, i])

    def v_in(i):
        return pltpu.make_async_copy(v_ref.at[pl.ds(i * per, per)], vbuf.at[i], ksem.at[1, i])

    get_x.wait()
    acc = None
    for j in range(parts):
        fetch(wq_ref, 0, 0, j).wait()
        fetch(wk_ref, 0, 1, j).wait()
        one = jnp.dot(x[:, j * step:(j + 1) * step], wbuf[j * step:(j + 1) * step, :], preferred_element_type=F32)
        acc = one if acc is None else acc + one
    g_ref[core, chip, :batch, :] = acc[:, :wide].astype(BF16)
    kv = jnp.where(core == 0, acc[:half, wide:], acc[half:, wide:])
    g_ref[core, chip, batch:, :] = kv.astype(BF16)

    @pl.loop(0, groups)
    def _(i):
        k_in(i).start()
        v_in(i).start()

    get_wo = pltpu.make_async_copy(wo_ref, wo, isem.at[2])
    get_wo.start()
    pl.semaphore_wait(barrier, len(offsets) + 1)

    def took(c, p):
        qf[pl.ds(c * chips + p, batch, stride=rows), :] = g_ref[c, p, :batch, :].astype(F32)
        at = (p // kv_heads) * batch * kv_heads + c * half * kv_heads + p % kv_heads
        kvf[pl.ds(at, half, stride=kv_heads), :] = g_ref[c, p, batch:, :].astype(F32)

    started = gather_blocks(lambda c, p: g_ref.at[c, p], chip, core, offsets, ahead, behind,
                            (asend, arecv, afsend, afrecv), took)
    get_pos.wait()

    cols = length * kv_heads
    lanes = per * rows
    lane = lax.broadcasted_iota(jnp.int32, (kv_heads, lanes), 1)
    sub = lax.broadcasted_iota(jnp.int32, (kv_heads, lanes), 0)
    ours = sub == ((lane % chips) * 2 * kv_heads // rows)
    member = lane // rows
    qlane = lax.broadcasted_iota(jnp.int32, (wide, lanes), 1) // rows
    slane = lax.broadcasted_iota(jnp.int32, (rows, wide), 1)

    zero = jnp.zeros((kv_heads, 2 * wide), BF16)

    def fresh(i, j, which):
        at = (which * batch + i * per + j) * kv_heads
        return kvf[pl.ds(pl.multiple_of(at, kv_heads), kv_heads), :].astype(BF16)

    def scores(i, slot):
        k_in(i).wait()
        for j in range(per):
            kn_ref[i * per + j] = fresh(i, j, 0)
        qt = qf[pl.ds(pl.multiple_of(i * lanes, lanes), lanes), :].T.astype(BF16)
        query = jnp.concatenate([jnp.where(qlane == j, qt, 0) for j in range(per)], axis=0)
        keys = jnp.concatenate([kbuf[i, j].reshape(cols, wide) for j in range(per)], axis=1)
        raw[slot, :cols, :] = jnp.dot(keys, query, preferred_element_type=F32)
        raw[slot, cols:, :] = jnp.dot(jnp.concatenate([fresh(i, j, 0) for j in range(per)], axis=1), query,
                                      preferred_element_type=F32)

    def soften(i, slot):
        end = jnp.zeros((kv_heads, lanes), jnp.int32)
        for j in range(per):
            end = jnp.where(member == j, pos[i * per + j] - base, end)
        scale = wide ** -0.5
        t = lax.broadcasted_iota(jnp.int32, (length, kv_heads, lanes), 0)
        s = raw[slot, :cols, :].reshape(length, kv_heads, lanes) * scale
        s = jnp.where(t < jnp.where(ours, end, 0)[None], s, -jnp.inf)
        newest = jnp.where(ours & (end >= 0) & (end < length), raw[slot, cols:, :] * scale, -jnp.inf)
        m = jnp.max(jnp.maximum(jnp.max(s, axis=0), newest), axis=0, keepdims=True)
        safe = jnp.where(m == -jnp.inf, 0.0, m)
        w = jnp.exp(s - safe[None])
        nw = jnp.exp(newest - safe)
        total = jnp.sum(jnp.sum(w, axis=0) + nw, axis=0, keepdims=True)
        wts[slot, :, :cols] = w.reshape(cols, lanes).T.astype(BF16)
        wts[slot, :, cols:] = jnp.concatenate([nw, jnp.zeros((wide - kv_heads, lanes), F32)], axis=0).T.astype(BF16)
        mls[slot] = jnp.concatenate([m, total, jnp.zeros((kv_heads - 2, lanes), F32)], axis=0).T

    def values(i, slot, stats):
        v_in(i).wait()
        at = (i // (groups // halves)) * rows * pitch + (i % (groups // halves)) * per
        for j in range(0, per, 2):
            vn0, vn1 = fresh(i, j, 1), fresh(i, j + 1, 1)
            vn_ref[i * per + j] = vn0
            vn_ref[i * per + j + 1] = vn1
            vals = jnp.concatenate([vbuf[i, j].reshape(cols, wide), vbuf[i, j + 1].reshape(cols, wide)], axis=1)
            vals = jnp.concatenate([vals, jnp.concatenate([vn0, vn1], axis=1), zero], axis=0)
            o = jnp.dot(wts[slot, j * rows:(j + 2) * rows, :cols + 2 * kv_heads], vals, preferred_element_type=F32)
            o_ref[pl.ds(at + j, rows, stride=pitch), :] = o[:rows, :wide]
            o_ref[pl.ds(at + j + 1, rows, stride=pitch), :] = o[rows:, wide:]
        for j in range(per):
            z = mls[slot, j * rows:(j + 1) * rows, :]
            stats = jnp.where(slane == i * per + j, z[:, 0:1], stats)
            stats = jnp.where(slane == batch + i * per + j, z[:, 1:2], stats)
        return stats

    def attend(p, stats):
        for c in range(2):
            stats = values(2 * p + c, c, stats)
            soften(2 * p + c + 1, 1 - c)
            scores(2 * p + c + 2, c)
        return stats

    def other(v):
        return pltpu.roll(v, batch, 1)

    def swap(t):
        return remote(o_ref.at[pl.ds(pl.multiple_of((t * 2 + 1 - core) * chips * pitch, chips * pitch), chips * pitch)],
                      theirs.at[t], xs.at[t], xr.at[t], partner)

    mlane = lax.broadcasted_iota(jnp.int32, (chips, wide), 1)

    def merge_pair(t):
        swap(t).wait_recv()
        first = pl.multiple_of((t * 2 + core) * chips * pitch, chips * pitch)
        sa = o_ref[pl.ds(first + share, chips, stride=pitch), :]
        sb = theirs[t, pl.ds(share, chips, stride=pitch), :]
        m = jnp.maximum(sa, sb)
        safe = jnp.where(m == -jnp.inf, 0.0, m)
        wa, wb = jnp.exp(sa - safe), jnp.exp(sb - safe)
        total = other(sa) * wa + other(sb) * wb
        mine[t, pl.ds(share, chips, stride=pitch), :] = jnp.where(mlane < batch, m, other(total))
        wt = jnp.concatenate([wa, wb], axis=0).T
        mid = slice(t * share, (t + 1) * share)
        for p in range(chips):
            a = o_ref[pl.ds(first + p * pitch, share), :] * wt[mid, p:p + 1]
            b = theirs[t, p * pitch:p * pitch + share, :] * wt[mid, chips + p:chips + p + 1]
            mine[t, p * pitch:p * pitch + share, :] = a + b
        for d in offsets:
            to = ahead(d)
            cp = remote(slot(mine.at[t], to), slot(got.at[t], chip), s1.at[t, to], r1.at[t, chip], to * 2 + core)
            cp.start()
            started.append(cp)
        own = pl.ds(pl.multiple_of(chip * pitch, pitch), pitch)
        got[t, own, :] = mine[t, own, :]

    def slot(ref, p):
        size = ref.shape[0] // chips
        return ref.at[pl.ds(pl.multiple_of(p * size, size), size)]

    def merge_chips(t):
        for d in offsets:
            src = behind(d)
            remote(slot(got.at[t], src), slot(got.at[t], src), s1.at[t, src], r1.at[t, src], partner).wait_recv()
        s = got[t, pl.ds(share, chips, stride=pitch), :]
        w = jnp.exp(s - jnp.max(s, axis=0, keepdims=True))
        w = w / jnp.sum(other(s) * w, axis=0, keepdims=True)
        wt = w.T
        mid = slice(t * share, (t + 1) * share)
        out = got[t, :share, :] * wt[mid, 0:1]
        for p in range(1, chips):
            out = out + got[t, p * pitch:p * pitch + share, :] * wt[mid, p:p + 1]
        return out.astype(BF16)

    pairs = groups // 2
    none = jnp.zeros((rows, wide), F32)
    scores(0, 0)
    soften(0, 0)
    scores(1, 1)

    def finish(t, stats):
        o_ref[pl.ds(t * rows * pitch + share, rows, stride=pitch), :] = stats
        swap(t).start()

    finish(0, lax.fori_loop(0, pairs // 2, attend, none))
    stats = lax.fori_loop(pairs // 2, pairs - 1, attend, none)
    merge_pair(0)
    stats = values(groups - 2, 0, stats)
    soften(groups - 1, 1)
    finish(1, values(groups - 1, 1, stats))
    merge_pair(1)
    out = jnp.concatenate([merge_chips(t) for t in range(halves)], axis=0)
    get_wo.wait()
    for p in range(chips):
        r = jnp.dot(out, wo[:, p * 2 * wide:(p + 1) * 2 * wide], preferred_element_type=F32)
        part[0, p * batch:(p + 1) * batch, :] = r[:, :wide]
        part[1, p * batch:(p + 1) * batch, :] = r[:, wide:]
    swap2 = remote(part.at[1 - core], ptheirs, xs.at[halves], xr.at[halves], partner)
    swap2.start()
    swap2.wait_recv()
    pmine[...] = part[core] + ptheirs[...]
    for d in offsets:
        to = ahead(d)
        cp = remote(slot(pmine, to), slot(pgot, chip), s2.at[to], r2.at[chip], to * 2 + core)
        cp.start()
        started.append(cp)
    own = pl.ds(pl.multiple_of(chip * batch, batch), batch)
    pgot[own, :] = pmine[own, :]
    for d in offsets:
        src = behind(d)
        remote(slot(pgot, src), slot(pgot, src), s2.at[src], r2.at[src], partner).wait_recv()
    y = pgot[:batch, :]
    for p in range(1, chips):
        y = y + pgot[p * batch:(p + 1) * batch, :]
    y_ref[:, pl.ds(pl.multiple_of(me * wide, wide), wide)] = y.astype(BF16)

    def block(c, p):
        return y_ref.at[:, pl.ds(pl.multiple_of((p * 2 + c) * wide, wide), wide)]

    started += gather_blocks(block, chip, core, offsets, ahead, behind, (send, recv, fsend, frecv))
    for t in range(halves):
        swap(t).wait_send()
    swap2.wait_send()
    for cp in started:
        cp.wait_send()


def store_kernel(pos_ref, k_ref, v_ref, kn_ref, vn_ref, y_ref, ko_ref, vo_ref, yo_ref, sem, rsem, ysem):
    batch, length = k_ref.shape[:2]
    chunks = sem.shape[1]
    per = batch // chunks
    base = lax.axis_index('seq') * length

    def whole(src, dst, a, i):
        return pltpu.make_async_copy(src.at[pl.ds(i * per, per)], dst.at[pl.ds(i * per, per)], sem.at[a, i])

    def row(src, dst, a, b):
        at = jnp.clip(pos_ref[b] - base, 0, length - 1)
        return pltpu.make_async_copy(src.at[b], dst.at[b, at], rsem.at[a, b])

    def here(b):
        end = pos_ref[b] - base
        return (end >= 0) & (end < length)

    @pl.loop(0, chunks)
    def _(i):
        whole(k_ref, ko_ref, 0, i).start()
        whole(v_ref, vo_ref, 1, i).start()

    y = pltpu.make_async_copy(y_ref, yo_ref, ysem)
    y.start()

    @pl.loop(0, chunks)
    def _(i):
        whole(k_ref, ko_ref, 0, i).wait()
        whole(v_ref, vo_ref, 1, i).wait()
        for j in range(per):
            b = i * per + j

            @pl.when(here(b))
            def _():
                row(kn_ref, ko_ref, 0, b).start()
                row(vn_ref, vo_ref, 1, b).start()

    y.wait()

    @pl.loop(0, batch)
    def _(b):
        @pl.when(here(b))
        def _():
            row(kn_ref, ko_ref, 0, b).wait()
            row(vn_ref, vo_ref, 1, b).wait()


def solution(mesh):
    n = mesh.shape['seq']
    chips = n // 2
    cache_spec = P('rep', 'seq', None, None)
    in_specs = (P('rep', None), P(), P(), P(), P('seq', None), cache_spec, cache_spec, P('rep'))
    out_specs = (P('rep', None), cache_spec, cache_spec)
    vmem = pl.BlockSpec(memory_space=pltpu.VMEM)
    smem = pl.BlockSpec(memory_space=pltpu.SMEM)
    hbm = pl.BlockSpec(memory_space=pltpu.HBM)
    anywhere = pl.BlockSpec(memory_space=pl.ANY)

    def step(x, wq, wk, wv, wo, k, v, pos):
        batch, depth = x.shape
        length, kv_heads, wide = k.shape[1:]
        heads = wq.shape[1] // wide
        slots = DMA((chips,))
        per = 2 * wide // heads
        groups = batch // per
        halves = 2
        pitch = batch // halves + 8
        cache = VMEM((groups, per, length, kv_heads, wide), BF16)
        new = jax.ShapeDtypeStruct((batch, kv_heads, wide), BF16)
        y, kn, vn = pl.pallas_call(
            functools.partial(decode_kernel, n),
            out_shape=[jax.ShapeDtypeStruct((batch, depth), BF16), new, new],
            in_specs=[anywhere] * 8, out_specs=[vmem] * 3,
            scratch_shapes=[
                pltpu.SMEM((batch,), jnp.int32), VMEM((batch, depth), BF16), VMEM(wo.shape, BF16),
                VMEM((depth, 2 * wide), BF16), VMEM((2, chips, batch + batch // 2, wide), BF16), cache, cache,
                VMEM((batch * heads, wide), F32), VMEM((2 * batch * kv_heads, wide), F32),
                VMEM((2, (length + 1) * kv_heads, per * heads), F32),
                VMEM((2, per * heads, length * kv_heads + wide), BF16), VMEM((2, per * heads, kv_heads), F32),
                VMEM((halves * heads * pitch, wide), F32)]
            + [VMEM((halves, chips * pitch, wide), F32)] * 3 + [VMEM((2, chips * batch, wide), F32)]
            + [VMEM((chips * batch, wide), F32)] * 3 + [DMA((3,)), DMA((2, 4)), DMA((2, groups))] + [slots] * 4
            + [DMA((halves + 1,))] * 2 + [DMA((halves, chips))] * 2 + [slots] * 6,
            compiler_params=pltpu.CompilerParams(collective_id=0, has_side_effects=True, vmem_limit_bytes=45 << 20),
            cost_estimate=pl.CostEstimate(flops=10 ** 10, bytes_accessed=32 << 20, transcendentals=0),
            name='decode',
        )(*(pltpu.with_memory_space_constraint(a, pltpu.HBM) for a in (pos, x, wq, wk, wv, wo, k, v)))
        chunks = 16
        ko, vo, y = pl.pallas_call(
            store_kernel,
            out_shape=[jax.ShapeDtypeStruct(k.shape, k.dtype), jax.ShapeDtypeStruct(v.shape, v.dtype),
                       jax.ShapeDtypeStruct((batch, depth), BF16)],
            in_specs=[smem, anywhere, anywhere, vmem, vmem, vmem], out_specs=[hbm, hbm, hbm],
            scratch_shapes=[DMA((2, chunks)), DMA((2, batch)), DMA],
            compiler_params=pltpu.CompilerParams(vmem_limit_bytes=4 << 20),
            cost_estimate=pl.CostEstimate(flops=10 ** 8, bytes_accessed=32 << 20, transcendentals=0),
            name='store',
        )(pos, k, v, kn, vn, y)
        return y, ko, vo

    return jax.shard_map(step, mesh=mesh, in_specs=in_specs, out_specs=out_specs, check_vma=False)
```

```python
import functools
import math

import jax
import jax.numpy as jnp
from jax import lax
from jax.experimental import pallas as pl
from jax.experimental.pallas import tpu as pltpu
from jax.sharding import PartitionSpec as P

F32 = jnp.float32
BF16 = jnp.bfloat16
MESH = pl.DeviceIdType.MESH
VMEM = pltpu.VMEM
DMA = pltpu.SemaphoreType.DMA


def place(n):
    me = lax.axis_index('seq')
    chips = n // 2
    side = math.isqrt(chips)
    chip, core = me // 2, me % 2
    row, col = chip // side, chip % side

    def far(d):
        return min(d[0], side - d[0]) + min(d[1], side - d[1])

    offsets = [(dy, dx) for dy in range(side) for dx in range(side) if dy or dx]
    offsets.sort(key=far, reverse=True)

    def ahead(d):
        return ((row + d[0]) % side) * side + (col + d[1]) % side

    def behind(d):
        return ((row + side - d[0]) % side) * side + (col + side - d[1]) % side

    return me, chip, core, offsets, ahead, behind


def remote(src, dst, send, recv, device):
    return pltpu.make_async_remote_copy(src_ref=src, dst_ref=dst, send_sem=send, recv_sem=recv,
                                        device_id={'seq': device}, device_id_type=MESH)


def greet(core, chip, offsets, ahead):
    barrier = pltpu.get_barrier_semaphore()
    for d in offsets:
        pl.semaphore_signal(barrier, inc=1, device_id={'seq': ahead(d) * 2 + core}, device_id_type=MESH)
    pl.semaphore_signal(barrier, inc=1, device_id={'seq': chip * 2 + 1 - core}, device_id_type=MESH)
    return barrier


def gather_blocks(block, chip, core, offsets, ahead, behind, sems, took=None, between=None):
    send, recv, fsend, frecv = sems
    partner = chip * 2 + 1 - core
    started = []
    for d in offsets:
        cp = remote(block(core, chip), block(core, chip), send.at[ahead(d)], recv.at[chip], ahead(d) * 2 + core)
        cp.start()
        started.append(cp)
    cp = remote(block(core, chip), block(core, chip), fsend.at[chip], frecv.at[chip], partner)
    cp.start()
    started.append(cp)
    if took is not None:
        took(core, chip)
    for k, d in enumerate(offsets):
        if k == 5 and between is not None:
            started += between()
        src = behind(d)
        got = block(core, src)
        remote(got, got, send.at[src], recv.at[src], partner).wait_recv()
        cp = remote(got, got, fsend.at[src], frecv.at[src], partner)
        cp.start()
        started.append(cp)
        if took is not None:
            took(core, src)
    for src in [chip] + [behind(d) for d in offsets]:
        got = block(1 - core, src)
        remote(got, got, fsend.at[src], frecv.at[src], partner).wait_recv()
        if took is not None:
            took(1 - core, src)
    return started


def decode_kernel(n, pos_ref, x_ref, wq_ref, wk_ref, wv_ref, wo_ref, k_ref, v_ref, y_ref, kn_ref, vn_ref,
                  pos, x, wo, wbuf, g_ref, kbuf, vbuf, qf, kvf, raw, wts, mls, o_ref, theirs, mine, got, wcol, heads, part, ptheirs,
                  isem, wsem, ksem, asend, arecv, afsend, afrecv, xs, xr, s1, r1, s2, r2, s3, r3, send, recv, fsend, frecv):
    me, chip, core, offsets, ahead, behind = place(n)
    chips = n // 2
    partner = chip * 2 + 1 - core
    barrier = greet(core, chip, offsets, ahead)
    batch, depth = x.shape
    wide = wbuf.shape[1] // 2
    groups, per, length, kv_heads, _ = kbuf.shape
    rows = qf.shape[0] // batch
    half = batch // 2
    halves = theirs.shape[0]
    pitch = theirs.shape[1] // chips
    share = batch // halves
    base = me * length

    parts = wsem.shape[1]
    step = depth // parts

    def fetch(w_ref, block, side, j):
        return pltpu.make_async_copy(
            w_ref.at[pl.ds(j * step, step), pl.ds(pl.multiple_of(block * wide, wide), wide)],
            wbuf.at[pl.ds(j * step, step), pl.ds(side * wide, wide)], wsem.at[side, j])

    get_x = pltpu.make_async_copy(x_ref, x, isem.at[0])
    get_x.start()
    for j in range(parts):
        fetch(wq_ref, me, 0, j).start()

        @pl.when(chip < kv_heads)
        def _():
            fetch(wk_ref, chip % kv_heads, 1, j).start()

        @pl.when(chip >= kv_heads)
        def _():
            fetch(wv_ref, chip % kv_heads, 1, j).start()

    get_pos = pltpu.make_async_copy(pos_ref, pos, isem.at[1])
    get_pos.start()

    def k_in(i):
        return pltpu.make_async_copy(k_ref.at[pl.ds(i * per, per)], kbuf.at[i], ksem.at[0, i])

    def v_in(i):
        return pltpu.make_async_copy(v_ref.at[pl.ds(i * per, per)], vbuf.at[i], ksem.at[1, i])

    get_x.wait()
    acc = None
    for j in range(parts):
        fetch(wq_ref, 0, 0, j).wait()
        fetch(wk_ref, 0, 1, j).wait()
        one = jnp.dot(x[:, j * step:(j + 1) * step], wbuf[j * step:(j + 1) * step, :], preferred_element_type=F32)
        acc = one if acc is None else acc + one
    g_ref[core, chip, :batch, :] = acc[:, :wide].astype(BF16)
    kv = jnp.where(core == 0, acc[:half, wide:], acc[half:, wide:])
    g_ref[core, chip, batch:, :] = kv.astype(BF16)

    @pl.loop(0, groups)
    def _(i):
        k_in(i).start()
        v_in(i).start()

    get_wo = pltpu.make_async_copy(wo_ref, wo, isem.at[2])
    get_wo.start()
    pl.semaphore_wait(barrier, len(offsets) + 1)

    def took(c, p):
        qf[pl.ds(c * chips + p, batch, stride=rows), :] = g_ref[c, p, :batch, :].astype(F32)
        at = (p // kv_heads) * batch * kv_heads + c * half * kv_heads + p % kv_heads
        kvf[pl.ds(at, half, stride=kv_heads), :] = g_ref[c, p, batch:, :].astype(F32)

    def columns(p):
        return pl.ds(pl.multiple_of(p * 2 * wide, 2 * wide), 2 * wide)

    def spread():
        get_wo.wait()
        cps = []
        for d in offsets:
            to = ahead(d)
            cp = remote(wo.at[:, columns(to)], wcol.at[chip], s3.at[to], r3.at[chip], to * 2 + core)
            cp.start()
            cps.append(cp)
        wcol[chip] = wo[:, columns(chip)]
        return cps

    started = gather_blocks(lambda c, p: g_ref.at[c, p], chip, core, offsets, ahead, behind,
                            (asend, arecv, afsend, afrecv), took, spread)
    get_pos.wait()

    cols = length * kv_heads
    lanes = per * rows
    lane = lax.broadcasted_iota(jnp.int32, (kv_heads, lanes), 1)
    sub = lax.broadcasted_iota(jnp.int32, (kv_heads, lanes), 0)
    ours = sub == ((lane % chips) * 2 * kv_heads // rows)
    member = lane // rows
    qlane = lax.broadcasted_iota(jnp.int32, (wide, lanes), 1) // rows
    slane = lax.broadcasted_iota(jnp.int32, (rows, wide), 1)

    zero = jnp.zeros((kv_heads, 2 * wide), BF16)

    def fresh(i, j, which):
        at = (which * batch + i * per + j) * kv_heads
        return kvf[pl.ds(pl.multiple_of(at, kv_heads), kv_heads), :].astype(BF16)

    def scores(i, slot):
        k_in(i).wait()
        for j in range(per):
            kn_ref[i * per + j] = fresh(i, j, 0)
        qt = qf[pl.ds(pl.multiple_of(i * lanes, lanes), lanes), :].T.astype(BF16)
        query = jnp.concatenate([jnp.where(qlane == j, qt, 0) for j in range(per)], axis=0)
        keys = jnp.concatenate([kbuf[i, j].reshape(cols, wide) for j in range(per)], axis=1)
        raw[slot, :cols, :] = jnp.dot(keys, query, preferred_element_type=F32)
        raw[slot, cols:, :] = jnp.dot(jnp.concatenate([fresh(i, j, 0) for j in range(per)], axis=1), query,
                                      preferred_element_type=F32)

    def soften(i, slot):
        end = jnp.zeros((kv_heads, lanes), jnp.int32)
        for j in range(per):
            end = jnp.where(member == j, pos[i * per + j] - base, end)
        scale = wide ** -0.5
        t = lax.broadcasted_iota(jnp.int32, (length, kv_heads, lanes), 0)
        s = raw[slot, :cols, :].reshape(length, kv_heads, lanes) * scale
        s = jnp.where(t < jnp.where(ours, end, 0)[None], s, -jnp.inf)
        newest = jnp.where(ours & (end >= 0) & (end < length), raw[slot, cols:, :] * scale, -jnp.inf)
        m = jnp.max(jnp.maximum(jnp.max(s, axis=0), newest), axis=0, keepdims=True)
        safe = jnp.where(m == -jnp.inf, 0.0, m)
        w = jnp.exp(s - safe[None])
        nw = jnp.exp(newest - safe)
        total = jnp.sum(jnp.sum(w, axis=0) + nw, axis=0, keepdims=True)
        wts[slot, :, :cols] = w.reshape(cols, lanes).T.astype(BF16)
        wts[slot, :, cols:] = jnp.concatenate([nw, jnp.zeros((wide - kv_heads, lanes), F32)], axis=0).T.astype(BF16)
        mls[slot] = jnp.concatenate([m, total, jnp.zeros((kv_heads - 2, lanes), F32)], axis=0).T

    def values(i, slot, stats):
        v_in(i).wait()
        at = (i // (groups // halves)) * rows * pitch + (i % (groups // halves)) * per
        for j in range(0, per, 2):
            vn0, vn1 = fresh(i, j, 1), fresh(i, j + 1, 1)
            vn_ref[i * per + j] = vn0
            vn_ref[i * per + j + 1] = vn1
            vals = jnp.concatenate([vbuf[i, j].reshape(cols, wide), vbuf[i, j + 1].reshape(cols, wide)], axis=1)
            vals = jnp.concatenate([vals, jnp.concatenate([vn0, vn1], axis=1), zero], axis=0)
            o = jnp.dot(wts[slot, j * rows:(j + 2) * rows, :cols + 2 * kv_heads], vals, preferred_element_type=F32)
            o_ref[pl.ds(at + j, rows, stride=pitch), :] = o[:rows, :wide]
            o_ref[pl.ds(at + j + 1, rows, stride=pitch), :] = o[rows:, wide:]
        for j in range(per):
            z = mls[slot, j * rows:(j + 1) * rows, :]
            stats = jnp.where(slane == i * per + j, z[:, 0:1], stats)
            stats = jnp.where(slane == batch + i * per + j, z[:, 1:2], stats)
        return stats

    def attend(p, stats):
        for c in range(2):
            stats = values(2 * p + c, c, stats)
            soften(2 * p + c + 1, 1 - c)
            scores(2 * p + c + 2, c)
        return stats

    def other(v):
        return pltpu.roll(v, batch, 1)

    def swap(t):
        return remote(o_ref.at[pl.ds(pl.multiple_of((t * 2 + 1 - core) * chips * pitch, chips * pitch), chips * pitch)],
                      theirs.at[t], xs.at[t], xr.at[t], partner)

    mlane = lax.broadcasted_iota(jnp.int32, (chips, wide), 1)

    def merge_pair(t):
        swap(t).wait_recv()
        first = pl.multiple_of((t * 2 + core) * chips * pitch, chips * pitch)
        sa = o_ref[pl.ds(first + share, chips, stride=pitch), :]
        sb = theirs[t, pl.ds(share, chips, stride=pitch), :]
        m = jnp.maximum(sa, sb)
        safe = jnp.where(m == -jnp.inf, 0.0, m)
        wa, wb = jnp.exp(sa - safe), jnp.exp(sb - safe)
        total = other(sa) * wa + other(sb) * wb
        mine[t, pl.ds(share, chips, stride=pitch), :] = jnp.where(mlane < batch, m, other(total))
        wt = jnp.concatenate([wa, wb], axis=0).T
        mid = slice(t * share, (t + 1) * share)
        for p in range(chips):
            a = o_ref[pl.ds(first + p * pitch, share), :] * wt[mid, p:p + 1]
            b = theirs[t, p * pitch:p * pitch + share, :] * wt[mid, chips + p:chips + p + 1]
            mine[t, p * pitch:p * pitch + share, :] = a + b
        for d in offsets:
            to = ahead(d)
            cp = remote(slot(mine.at[t], to), slot(got.at[t], chip), s1.at[t, to], r1.at[t, chip], to * 2 + core)
            cp.start()
            started.append(cp)
        own = pl.ds(pl.multiple_of(chip * pitch, pitch), pitch)
        got[t, own, :] = mine[t, own, :]

    def slot(ref, p):
        size = ref.shape[0] // chips
        return ref.at[pl.ds(pl.multiple_of(p * size, size), size)]

    def merge_chips(t):
        for d in offsets:
            src = behind(d)
            remote(slot(got.at[t], src), slot(got.at[t], src), s1.at[t, src], r1.at[t, src], partner).wait_recv()
        s = got[t, pl.ds(share, chips, stride=pitch), :]
        w = jnp.exp(s - jnp.max(s, axis=0, keepdims=True))
        w = w / jnp.sum(other(s) * w, axis=0, keepdims=True)
        wt = w.T
        mid = slice(t * share, (t + 1) * share)
        out = got[t, :share, :] * wt[mid, 0:1]
        for p in range(1, chips):
            out = out + got[t, p * pitch:p * pitch + share, :] * wt[mid, p:p + 1]
        return out.astype(BF16)

    pairs = groups // 2
    none = jnp.zeros((rows, wide), F32)
    scores(0, 0)
    soften(0, 0)
    scores(1, 1)

    def finish(t, stats):
        o_ref[pl.ds(t * rows * pitch + share, rows, stride=pitch), :] = stats
        swap(t).start()

    finish(0, lax.fori_loop(0, pairs // 2, attend, none))
    stats = lax.fori_loop(pairs // 2, pairs - 1, attend, none)
    merge_pair(0)
    stats = values(groups - 2, 0, stats)
    soften(groups - 1, 1)
    finish(1, values(groups - 1, 1, stats))
    merge_pair(1)
    out = jnp.concatenate([merge_chips(t) for t in range(halves)], axis=0)
    heads[chip] = out
    for d in offsets:
        to = ahead(d)
        cp = remote(heads.at[chip], heads.at[chip], s2.at[to], r2.at[chip], to * 2 + core)
        cp.start()
        started.append(cp)
    for d in offsets:
        src = behind(d)
        remote(wcol.at[src], wcol.at[src], s3.at[src], r3.at[src], partner).wait_recv()
    for d in offsets:
        src = behind(d)
        remote(heads.at[src], heads.at[src], s2.at[src], r2.at[src], partner).wait_recv()
    y = jnp.dot(jnp.concatenate([heads[p] for p in range(chips)], axis=1), wcol[...].reshape(chips * wide, 2 * wide),
                preferred_element_type=F32)
    part[0] = y[:, :wide]
    part[1] = y[:, wide:]
    swap2 = remote(part.at[1 - core], ptheirs, xs.at[halves], xr.at[halves], partner)
    swap2.start()
    swap2.wait_recv()
    y = part[core] + ptheirs[...]
    y_ref[:, pl.ds(pl.multiple_of(me * wide, wide), wide)] = y.astype(BF16)

    def block(c, p):
        return y_ref.at[:, pl.ds(pl.multiple_of((p * 2 + c) * wide, wide), wide)]

    started += gather_blocks(block, chip, core, offsets, ahead, behind, (send, recv, fsend, frecv))
    for t in range(halves):
        swap(t).wait_send()
    swap2.wait_send()
    for cp in started:
        cp.wait_send()


def store_kernel(pos_ref, k_ref, v_ref, kn_ref, vn_ref, y_ref, ko_ref, vo_ref, yo_ref, sem, rsem, ysem):
    batch, length = k_ref.shape[:2]
    chunks = sem.shape[1]
    per = batch // chunks
    base = lax.axis_index('seq') * length

    def whole(src, dst, a, i):
        return pltpu.make_async_copy(src.at[pl.ds(i * per, per)], dst.at[pl.ds(i * per, per)], sem.at[a, i])

    def row(src, dst, a, b):
        at = jnp.clip(pos_ref[b] - base, 0, length - 1)
        return pltpu.make_async_copy(src.at[b], dst.at[b, at], rsem.at[a, b])

    def here(b):
        end = pos_ref[b] - base
        return (end >= 0) & (end < length)

    @pl.loop(0, chunks)
    def _(i):
        whole(k_ref, ko_ref, 0, i).start()
        whole(v_ref, vo_ref, 1, i).start()

    y = pltpu.make_async_copy(y_ref, yo_ref, ysem)
    y.start()

    @pl.loop(0, chunks)
    def _(i):
        whole(k_ref, ko_ref, 0, i).wait()
        whole(v_ref, vo_ref, 1, i).wait()
        for j in range(per):
            b = i * per + j

            @pl.when(here(b))
            def _():
                row(kn_ref, ko_ref, 0, b).start()
                row(vn_ref, vo_ref, 1, b).start()

    y.wait()

    @pl.loop(0, batch)
    def _(b):
        @pl.when(here(b))
        def _():
            row(kn_ref, ko_ref, 0, b).wait()
            row(vn_ref, vo_ref, 1, b).wait()


def solution(mesh):
    n = mesh.shape['seq']
    chips = n // 2
    cache_spec = P('rep', 'seq', None, None)
    in_specs = (P('rep', None), P(), P(), P(), P('seq', None), cache_spec, cache_spec, P('rep'))
    out_specs = (P('rep', None), cache_spec, cache_spec)
    vmem = pl.BlockSpec(memory_space=pltpu.VMEM)
    smem = pl.BlockSpec(memory_space=pltpu.SMEM)
    hbm = pl.BlockSpec(memory_space=pltpu.HBM)
    anywhere = pl.BlockSpec(memory_space=pl.ANY)

    def step(x, wq, wk, wv, wo, k, v, pos):
        batch, depth = x.shape
        length, kv_heads, wide = k.shape[1:]
        heads = wq.shape[1] // wide
        slots = DMA((chips,))
        per = 2 * wide // heads
        groups = batch // per
        halves = 2
        pitch = batch // halves + 8
        cache = VMEM((groups, per, length, kv_heads, wide), BF16)
        new = jax.ShapeDtypeStruct((batch, kv_heads, wide), BF16)
        y, kn, vn = pl.pallas_call(
            functools.partial(decode_kernel, n),
            out_shape=[jax.ShapeDtypeStruct((batch, depth), BF16), new, new],
            in_specs=[anywhere] * 8, out_specs=[vmem] * 3,
            scratch_shapes=[
                pltpu.SMEM((batch,), jnp.int32), VMEM((batch, depth), BF16), VMEM(wo.shape, BF16),
                VMEM((depth, 2 * wide), BF16), VMEM((2, chips, batch + batch // 2, wide), BF16), cache, cache,
                VMEM((batch * heads, wide), F32), VMEM((2 * batch * kv_heads, wide), F32),
                VMEM((2, (length + 1) * kv_heads, per * heads), F32),
                VMEM((2, per * heads, length * kv_heads + wide), BF16), VMEM((2, per * heads, kv_heads), F32),
                VMEM((halves * heads * pitch, wide), F32)]
            + [VMEM((halves, chips * pitch, wide), F32)] * 3
            + [VMEM((chips, wide, 2 * wide), BF16), VMEM((chips, batch, wide), BF16), VMEM((2, batch, wide), F32),
               VMEM((batch, wide), F32)] + [DMA((3,)), DMA((2, 4)), DMA((2, groups))] + [slots] * 4
            + [DMA((halves + 1,))] * 2 + [DMA((halves, chips))] * 2 + [slots] * 8,
            compiler_params=pltpu.CompilerParams(collective_id=0, has_side_effects=True, vmem_limit_bytes=45 << 20),
            cost_estimate=pl.CostEstimate(flops=10 ** 10, bytes_accessed=32 << 20, transcendentals=0),
            name='decode',
        )(*(pltpu.with_memory_space_constraint(a, pltpu.HBM) for a in (pos, x, wq, wk, wv, wo, k, v)))
        chunks = 16
        ko, vo, y = pl.pallas_call(
            store_kernel,
            out_shape=[jax.ShapeDtypeStruct(k.shape, k.dtype), jax.ShapeDtypeStruct(v.shape, v.dtype),
                       jax.ShapeDtypeStruct((batch, depth), BF16)],
            in_specs=[smem, anywhere, anywhere, vmem, vmem, vmem], out_specs=[hbm, hbm, hbm],
            scratch_shapes=[DMA((2, chunks)), DMA((2, batch)), DMA],
            compiler_params=pltpu.CompilerParams(vmem_limit_bytes=4 << 20),
            cost_estimate=pl.CostEstimate(flops=10 ** 8, bytes_accessed=32 << 20, transcendentals=0),
            name='store',
        )(pos, k, v, kn, vn, y)
        return y, ko, vo

    return jax.shard_map(step, mesh=mesh, in_specs=in_specs, out_specs=out_specs, check_vma=False)
```

```python
import functools
import math

import jax
import jax.numpy as jnp
from jax import lax
from jax.experimental import pallas as pl
from jax.experimental.pallas import tpu as pltpu
from jax.sharding import PartitionSpec as P

F32 = jnp.float32
BF16 = jnp.bfloat16
MESH = pl.DeviceIdType.MESH
VMEM = pltpu.VMEM
DMA = pltpu.SemaphoreType.DMA


def place(n):
    me = lax.axis_index('seq')
    chips = n // 2
    side = math.isqrt(chips)
    chip, core = me // 2, me % 2
    row, col = chip // side, chip % side

    def far(d):
        return min(d[0], side - d[0]) + min(d[1], side - d[1])

    offsets = [(dy, dx) for dy in range(side) for dx in range(side) if dy or dx]
    offsets.sort(key=far, reverse=True)

    def ahead(d):
        return ((row + d[0]) % side) * side + (col + d[1]) % side

    def behind(d):
        return ((row + side - d[0]) % side) * side + (col + side - d[1]) % side

    return me, chip, core, offsets, ahead, behind


def remote(src, dst, send, recv, device):
    return pltpu.make_async_remote_copy(src_ref=src, dst_ref=dst, send_sem=send, recv_sem=recv,
                                        device_id={'seq': device}, device_id_type=MESH)


def greet(core, chip, offsets, ahead):
    barrier = pltpu.get_barrier_semaphore()
    for d in offsets:
        pl.semaphore_signal(barrier, inc=1, device_id={'seq': ahead(d) * 2 + core}, device_id_type=MESH)
    pl.semaphore_signal(barrier, inc=1, device_id={'seq': chip * 2 + 1 - core}, device_id_type=MESH)
    return barrier


def gather_blocks(block, chip, core, offsets, ahead, behind, sems, took=None, between=None):
    send, recv, fsend, frecv = sems
    partner = chip * 2 + 1 - core
    started = []
    for d in offsets:
        cp = remote(block(core, chip), block(core, chip), send.at[ahead(d)], recv.at[chip], ahead(d) * 2 + core)
        cp.start()
        started.append(cp)
    cp = remote(block(core, chip), block(core, chip), fsend.at[chip], frecv.at[chip], partner)
    cp.start()
    started.append(cp)
    if took is not None:
        took(core, chip)
    for k, d in enumerate(reversed(offsets)):
        if k == 5 and between is not None:
            started += between()
        src = behind(d)
        got = block(core, src)
        remote(got, got, send.at[src], recv.at[src], partner).wait_recv()
        cp = remote(got, got, fsend.at[src], frecv.at[src], partner)
        cp.start()
        started.append(cp)
        if took is not None:
            took(core, src)
    for src in [chip] + [behind(d) for d in reversed(offsets)]:
        got = block(1 - core, src)
        remote(got, got, fsend.at[src], frecv.at[src], partner).wait_recv()
        if took is not None:
            took(1 - core, src)
    return started


def decode_kernel(n, pos_ref, x_ref, wq_ref, wk_ref, wv_ref, wo_ref, k_ref, v_ref, y_ref, kn_ref, vn_ref,
                  pos, x, wo, wbuf, g_ref, kbuf, vbuf, qf, kvf, raw, wts, mls, o_ref, theirs, mine, got, wcol, heads, part, ptheirs,
                  isem, wsem, ksem, asend, arecv, afsend, afrecv, xs, xr, s1, r1, s2, r2, s3, r3, send, recv, fsend, frecv):
    me, chip, core, offsets, ahead, behind = place(n)
    chips = n // 2
    partner = chip * 2 + 1 - core
    barrier = greet(core, chip, offsets, ahead)
    batch, depth = x.shape
    wide = wbuf.shape[1] // 2
    groups, per, length, kv_heads, _ = kbuf.shape
    rows = qf.shape[0] // batch
    half = batch // 2
    halves = theirs.shape[0]
    pitch = theirs.shape[1] // chips
    share = batch // halves
    base = me * length

    parts = wsem.shape[1]
    step = depth // parts

    def fetch(w_ref, block, side, j):
        return pltpu.make_async_copy(
            w_ref.at[pl.ds(j * step, step), pl.ds(pl.multiple_of(block * wide, wide), wide)],
            wbuf.at[pl.ds(j * step, step), pl.ds(side * wide, wide)], wsem.at[side, j])

    get_x = pltpu.make_async_copy(x_ref, x, isem.at[0])
    get_x.start()
    for j in range(parts):
        fetch(wq_ref, me, 0, j).start()

        @pl.when(chip < kv_heads)
        def _():
            fetch(wk_ref, chip % kv_heads, 1, j).start()

        @pl.when(chip >= kv_heads)
        def _():
            fetch(wv_ref, chip % kv_heads, 1, j).start()

    get_pos = pltpu.make_async_copy(pos_ref, pos, isem.at[1])
    get_pos.start()

    def k_in(i):
        return pltpu.make_async_copy(k_ref.at[pl.ds(i * per, per)], kbuf.at[i], ksem.at[0, i])

    def v_in(i):
        return pltpu.make_async_copy(v_ref.at[pl.ds(i * per, per)], vbuf.at[i], ksem.at[1, i])

    get_x.wait()
    acc = None
    for j in range(parts):
        fetch(wq_ref, 0, 0, j).wait()
        fetch(wk_ref, 0, 1, j).wait()
        one = jnp.dot(x[:, j * step:(j + 1) * step], wbuf[j * step:(j + 1) * step, :], preferred_element_type=F32)
        acc = one if acc is None else acc + one
    g_ref[core, chip, :batch, :] = acc[:, :wide].astype(BF16)
    kv = jnp.where(core == 0, acc[:half, wide:], acc[half:, wide:])
    g_ref[core, chip, batch:, :] = kv.astype(BF16)

    @pl.loop(0, groups)
    def _(i):
        k_in(i).start()
        v_in(i).start()

    get_wo = pltpu.make_async_copy(wo_ref, wo, isem.at[2])
    get_wo.start()
    pl.semaphore_wait(barrier, len(offsets) + 1)

    def took(c, p):
        qf[pl.ds(c * chips + p, batch, stride=rows), :] = g_ref[c, p, :batch, :].astype(F32)
        at = (p // kv_heads) * batch * kv_heads + c * half * kv_heads + p % kv_heads
        kvf[pl.ds(at, half, stride=kv_heads), :] = g_ref[c, p, batch:, :].astype(F32)

    def columns(p):
        return pl.ds(pl.multiple_of(p * 2 * wide, 2 * wide), 2 * wide)

    def spread():
        get_wo.wait()
        cps = []
        for d in offsets:
            to = ahead(d)
            cp = remote(wo.at[:, columns(to)], wcol.at[chip], s3.at[to], r3.at[chip], to * 2 + core)
            cp.start()
            cps.append(cp)
        wcol[chip] = wo[:, columns(chip)]
        return cps

    started = gather_blocks(lambda c, p: g_ref.at[c, p], chip, core, offsets, ahead, behind,
                            (asend, arecv, afsend, afrecv), took, spread)
    get_pos.wait()

    cols = length * kv_heads
    lanes = per * rows
    lane = lax.broadcasted_iota(jnp.int32, (kv_heads, lanes), 1)
    sub = lax.broadcasted_iota(jnp.int32, (kv_heads, lanes), 0)
    ours = sub == ((lane % chips) * 2 * kv_heads // rows)
    member = lane // rows
    qlane = lax.broadcasted_iota(jnp.int32, (wide, lanes), 1) // rows
    slane = lax.broadcasted_iota(jnp.int32, (rows, wide), 1)

    zero = jnp.zeros((kv_heads, 2 * wide), BF16)

    def fresh(i, j, which):
        at = (which * batch + i * per + j) * kv_heads
        return kvf[pl.ds(pl.multiple_of(at, kv_heads), kv_heads), :].astype(BF16)

    def scores(i, slot):
        k_in(i).wait()
        for j in range(per):
            kn_ref[i * per + j] = fresh(i, j, 0)
        qt = qf[pl.ds(pl.multiple_of(i * lanes, lanes), lanes), :].T.astype(BF16)
        query = jnp.concatenate([jnp.where(qlane == j, qt, 0) for j in range(per)], axis=0)
        keys = jnp.concatenate([kbuf[i, j].reshape(cols, wide) for j in range(per)], axis=1)
        raw[slot, :cols, :] = jnp.dot(keys, query, preferred_element_type=F32)
        raw[slot, cols:, :] = jnp.dot(jnp.concatenate([fresh(i, j, 0) for j in range(per)], axis=1), query,
                                      preferred_element_type=F32)

    def soften(i, slot):
        end = jnp.zeros((kv_heads, lanes), jnp.int32)
        for j in range(per):
            end = jnp.where(member == j, pos[i * per + j] - base, end)
        scale = wide ** -0.5
        t = lax.broadcasted_iota(jnp.int32, (length, kv_heads, lanes), 0)
        s = raw[slot, :cols, :].reshape(length, kv_heads, lanes) * scale
        s = jnp.where(t < jnp.where(ours, end, 0)[None], s, -jnp.inf)
        newest = jnp.where(ours & (end >= 0) & (end < length), raw[slot, cols:, :] * scale, -jnp.inf)
        m = jnp.max(jnp.maximum(jnp.max(s, axis=0), newest), axis=0, keepdims=True)
        safe = jnp.where(m == -jnp.inf, 0.0, m)
        w = jnp.exp(s - safe[None])
        nw = jnp.exp(newest - safe)
        total = jnp.sum(jnp.sum(w, axis=0) + nw, axis=0, keepdims=True)
        wts[slot, :, :cols] = w.reshape(cols, lanes).T.astype(BF16)
        wts[slot, :, cols:] = jnp.concatenate([nw, jnp.zeros((wide - kv_heads, lanes), F32)], axis=0).T.astype(BF16)
        mls[slot] = jnp.concatenate([m, total, jnp.zeros((kv_heads - 2, lanes), F32)], axis=0).T

    def values(i, slot, stats):
        v_in(i).wait()
        at = (i // (groups // halves)) * rows * pitch + (i % (groups // halves)) * per
        for j in range(0, per, 2):
            vn0, vn1 = fresh(i, j, 1), fresh(i, j + 1, 1)
            vn_ref[i * per + j] = vn0
            vn_ref[i * per + j + 1] = vn1
            vals = jnp.concatenate([vbuf[i, j].reshape(cols, wide), vbuf[i, j + 1].reshape(cols, wide)], axis=1)
            vals = jnp.concatenate([vals, jnp.concatenate([vn0, vn1], axis=1), zero], axis=0)
            o = jnp.dot(wts[slot, j * rows:(j + 2) * rows, :cols + 2 * kv_heads], vals, preferred_element_type=F32)
            o_ref[pl.ds(at + j, rows, stride=pitch), :] = o[:rows, :wide]
            o_ref[pl.ds(at + j + 1, rows, stride=pitch), :] = o[rows:, wide:]
        for j in range(per):
            z = mls[slot, j * rows:(j + 1) * rows, :]
            stats = jnp.where(slane == i * per + j, z[:, 0:1], stats)
            stats = jnp.where(slane == batch + i * per + j, z[:, 1:2], stats)
        return stats

    def attend(p, stats):
        for c in range(2):
            stats = values(2 * p + c, c, stats)
            soften(2 * p + c + 1, 1 - c)
            scores(2 * p + c + 2, c)
        return stats

    def other(v):
        return pltpu.roll(v, batch, 1)

    def swap(t):
        return remote(o_ref.at[pl.ds(pl.multiple_of((t * 2 + 1 - core) * chips * pitch, chips * pitch), chips * pitch)],
                      theirs.at[t], xs.at[t], xr.at[t], partner)

    mlane = lax.broadcasted_iota(jnp.int32, (chips, wide), 1)

    def merge_pair(t):
        swap(t).wait_recv()
        first = pl.multiple_of((t * 2 + core) * chips * pitch, chips * pitch)
        sa = o_ref[pl.ds(first + share, chips, stride=pitch), :]
        sb = theirs[t, pl.ds(share, chips, stride=pitch), :]
        m = jnp.maximum(sa, sb)
        safe = jnp.where(m == -jnp.inf, 0.0, m)
        wa, wb = jnp.exp(sa - safe), jnp.exp(sb - safe)
        total = other(sa) * wa + other(sb) * wb
        mine[t, pl.ds(share, chips, stride=pitch), :] = jnp.where(mlane < batch, m, other(total))
        wt = jnp.concatenate([wa, wb], axis=0).T
        mid = slice(t * share, (t + 1) * share)
        for p in range(chips):
            a = o_ref[pl.ds(first + p * pitch, share), :] * wt[mid, p:p + 1]
            b = theirs[t, p * pitch:p * pitch + share, :] * wt[mid, chips + p:chips + p + 1]
            mine[t, p * pitch:p * pitch + share, :] = a + b
        for d in offsets:
            to = ahead(d)
            cp = remote(slot(mine.at[t], to), slot(got.at[t], chip), s1.at[t, to], r1.at[t, chip], to * 2 + core)
            cp.start()
            started.append(cp)
        own = pl.ds(pl.multiple_of(chip * pitch, pitch), pitch)
        got[t, own, :] = mine[t, own, :]

    def slot(ref, p):
        size = ref.shape[0] // chips
        return ref.at[pl.ds(pl.multiple_of(p * size, size), size)]

    def merge_chips(t):
        for d in offsets:
            src = behind(d)
            remote(slot(got.at[t], src), slot(got.at[t], src), s1.at[t, src], r1.at[t, src], partner).wait_recv()
        s = got[t, pl.ds(share, chips, stride=pitch), :]
        w = jnp.exp(s - jnp.max(s, axis=0, keepdims=True))
        w = w / jnp.sum(other(s) * w, axis=0, keepdims=True)
        wt = w.T
        mid = slice(t * share, (t + 1) * share)
        out = got[t, :share, :] * wt[mid, 0:1]
        for p in range(1, chips):
            out = out + got[t, p * pitch:p * pitch + share, :] * wt[mid, p:p + 1]
        return out.astype(BF16)

    pairs = groups // 2
    none = jnp.zeros((rows, wide), F32)
    scores(0, 0)
    soften(0, 0)
    scores(1, 1)

    def finish(t, stats):
        o_ref[pl.ds(t * rows * pitch + share, rows, stride=pitch), :] = stats
        swap(t).start()

    finish(0, lax.fori_loop(0, pairs // 2, attend, none))
    stats = lax.fori_loop(pairs // 2, pairs - 1, attend, none)
    merge_pair(0)
    stats = values(groups - 2, 0, stats)
    soften(groups - 1, 1)
    finish(1, values(groups - 1, 1, stats))
    merge_pair(1)
    out = jnp.concatenate([merge_chips(t) for t in range(halves)], axis=0)
    heads[chip] = out
    for d in offsets:
        to = ahead(d)
        cp = remote(heads.at[chip], heads.at[chip], s2.at[to], r2.at[chip], to * 2 + core)
        cp.start()
        started.append(cp)
    for d in offsets:
        src = behind(d)
        remote(wcol.at[src], wcol.at[src], s3.at[src], r3.at[src], partner).wait_recv()
    for d in offsets:
        src = behind(d)
        remote(heads.at[src], heads.at[src], s2.at[src], r2.at[src], partner).wait_recv()
    y = jnp.dot(jnp.concatenate([heads[p] for p in range(chips)], axis=1), wcol[...].reshape(chips * wide, 2 * wide),
                preferred_element_type=F32)
    part[0] = y[:, :wide]
    part[1] = y[:, wide:]
    swap2 = remote(part.at[1 - core], ptheirs, xs.at[halves], xr.at[halves], partner)
    swap2.start()
    swap2.wait_recv()
    y = part[core] + ptheirs[...]
    y_ref[:, pl.ds(pl.multiple_of(me * wide, wide), wide)] = y.astype(BF16)

    def block(c, p):
        return y_ref.at[:, pl.ds(pl.multiple_of((p * 2 + c) * wide, wide), wide)]

    started += gather_blocks(block, chip, core, offsets, ahead, behind, (send, recv, fsend, frecv))
    for t in range(halves):
        swap(t).wait_send()
    swap2.wait_send()
    for cp in started:
        cp.wait_send()


def store_kernel(pos_ref, k_ref, v_ref, kn_ref, vn_ref, y_ref, ko_ref, vo_ref, yo_ref, sem, rsem, ysem):
    batch, length = k_ref.shape[:2]
    chunks = sem.shape[1]
    per = batch // chunks
    base = lax.axis_index('seq') * length

    def whole(src, dst, a, i):
        return pltpu.make_async_copy(src.at[pl.ds(i * per, per)], dst.at[pl.ds(i * per, per)], sem.at[a, i])

    def row(src, dst, a, b):
        at = jnp.clip(pos_ref[b] - base, 0, length - 1)
        return pltpu.make_async_copy(src.at[b], dst.at[b, at], rsem.at[a, b])

    def here(b):
        end = pos_ref[b] - base
        return (end >= 0) & (end < length)

    @pl.loop(0, chunks)
    def _(i):
        whole(k_ref, ko_ref, 0, i).start()
        whole(v_ref, vo_ref, 1, i).start()

    y = pltpu.make_async_copy(y_ref, yo_ref, ysem)
    y.start()

    @pl.loop(0, chunks)
    def _(i):
        whole(k_ref, ko_ref, 0, i).wait()
        whole(v_ref, vo_ref, 1, i).wait()
        for j in range(per):
            b = i * per + j

            @pl.when(here(b))
            def _():
                row(kn_ref, ko_ref, 0, b).start()
                row(vn_ref, vo_ref, 1, b).start()

    y.wait()

    @pl.loop(0, batch)
    def _(b):
        @pl.when(here(b))
        def _():
            row(kn_ref, ko_ref, 0, b).wait()
            row(vn_ref, vo_ref, 1, b).wait()


def solution(mesh):
    n = mesh.shape['seq']
    chips = n // 2
    cache_spec = P('rep', 'seq', None, None)
    in_specs = (P('rep', None), P(), P(), P(), P('seq', None), cache_spec, cache_spec, P('rep'))
    out_specs = (P('rep', None), cache_spec, cache_spec)
    vmem = pl.BlockSpec(memory_space=pltpu.VMEM)
    smem = pl.BlockSpec(memory_space=pltpu.SMEM)
    hbm = pl.BlockSpec(memory_space=pltpu.HBM)
    anywhere = pl.BlockSpec(memory_space=pl.ANY)

    def step(x, wq, wk, wv, wo, k, v, pos):
        batch, depth = x.shape
        length, kv_heads, wide = k.shape[1:]
        heads = wq.shape[1] // wide
        slots = DMA((chips,))
        per = 2 * wide // heads
        groups = batch // per
        halves = 2
        pitch = batch // halves + 8
        cache = VMEM((groups, per, length, kv_heads, wide), BF16)
        new = jax.ShapeDtypeStruct((batch, kv_heads, wide), BF16)
        y, kn, vn = pl.pallas_call(
            functools.partial(decode_kernel, n),
            out_shape=[jax.ShapeDtypeStruct((batch, depth), BF16), new, new],
            in_specs=[anywhere] * 8, out_specs=[vmem] * 3,
            scratch_shapes=[
                pltpu.SMEM((batch,), jnp.int32), VMEM((batch, depth), BF16), VMEM(wo.shape, BF16),
                VMEM((depth, 2 * wide), BF16), VMEM((2, chips, batch + batch // 2, wide), BF16), cache, cache,
                VMEM((batch * heads, wide), F32), VMEM((2 * batch * kv_heads, wide), F32),
                VMEM((2, (length + 1) * kv_heads, per * heads), F32),
                VMEM((2, per * heads, length * kv_heads + wide), BF16), VMEM((2, per * heads, kv_heads), F32),
                VMEM((halves * heads * pitch, wide), F32)]
            + [VMEM((halves, chips * pitch, wide), F32)] * 3
            + [VMEM((chips, wide, 2 * wide), BF16), VMEM((chips, batch, wide), BF16), VMEM((2, batch, wide), F32),
               VMEM((batch, wide), F32)] + [DMA((3,)), DMA((2, 4)), DMA((2, groups))] + [slots] * 4
            + [DMA((halves + 1,))] * 2 + [DMA((halves, chips))] * 2 + [slots] * 8,
            compiler_params=pltpu.CompilerParams(collective_id=0, has_side_effects=True, vmem_limit_bytes=45 << 20),
            cost_estimate=pl.CostEstimate(flops=10 ** 10, bytes_accessed=32 << 20, transcendentals=0),
            name='decode',
        )(*(pltpu.with_memory_space_constraint(a, pltpu.HBM) for a in (pos, x, wq, wk, wv, wo, k, v)))
        chunks = 16
        ko, vo, y = pl.pallas_call(
            store_kernel,
            out_shape=[jax.ShapeDtypeStruct(k.shape, k.dtype), jax.ShapeDtypeStruct(v.shape, v.dtype),
                       jax.ShapeDtypeStruct((batch, depth), BF16)],
            in_specs=[smem, anywhere, anywhere, vmem, vmem, vmem], out_specs=[hbm, hbm, hbm],
            scratch_shapes=[DMA((2, chunks)), DMA((2, batch)), DMA],
            compiler_params=pltpu.CompilerParams(vmem_limit_bytes=4 << 20),
            cost_estimate=pl.CostEstimate(flops=10 ** 8, bytes_accessed=32 << 20, transcendentals=0),
            name='store',
        )(pos, k, v, kn, vn, y)
        return y, ko, vo

    return jax.shard_map(step, mesh=mesh, in_specs=in_specs, out_specs=out_specs, check_vma=False)
```

```python
import functools
import math

import jax
import jax.numpy as jnp
from jax import lax
from jax.experimental import pallas as pl
from jax.experimental.pallas import tpu as pltpu
from jax.sharding import PartitionSpec as P

F32 = jnp.float32
BF16 = jnp.bfloat16
MESH = pl.DeviceIdType.MESH
VMEM = pltpu.VMEM
DMA = pltpu.SemaphoreType.DMA


def place(n):
    me = lax.axis_index('seq')
    chips = n // 2
    side = math.isqrt(chips)
    chip, core = me // 2, me % 2
    row, col = chip // side, chip % side

    def far(d):
        return min(d[0], side - d[0]) + min(d[1], side - d[1])

    offsets = [(dy, dx) for dy in range(side) for dx in range(side) if dy or dx]
    offsets.sort(key=far, reverse=True)

    def ahead(d):
        return ((row + d[0]) % side) * side + (col + d[1]) % side

    def behind(d):
        return ((row + side - d[0]) % side) * side + (col + side - d[1]) % side

    return me, chip, core, offsets, ahead, behind


def remote(src, dst, send, recv, device):
    return pltpu.make_async_remote_copy(src_ref=src, dst_ref=dst, send_sem=send, recv_sem=recv,
                                        device_id={'seq': device}, device_id_type=MESH)


def greet(core, chip, offsets, ahead):
    barrier = pltpu.get_barrier_semaphore()
    for d in offsets:
        pl.semaphore_signal(barrier, inc=1, device_id={'seq': ahead(d) * 2 + core}, device_id_type=MESH)
    pl.semaphore_signal(barrier, inc=1, device_id={'seq': chip * 2 + 1 - core}, device_id_type=MESH)
    return barrier


def gather_blocks(block, chip, core, offsets, ahead, behind, sems, took=None, between=None):
    send, recv, fsend, frecv = sems
    partner = chip * 2 + 1 - core
    started = []
    for d in offsets:
        cp = remote(block(core, chip), block(core, chip), send.at[ahead(d)], recv.at[chip], ahead(d) * 2 + core)
        cp.start()
        started.append(cp)
    cp = remote(block(core, chip), block(core, chip), fsend.at[chip], frecv.at[chip], partner)
    cp.start()
    started.append(cp)
    if took is not None:
        took(core, chip)
    for k, d in enumerate(reversed(offsets)):
        if k == 5 and between is not None:
            started += between()
        src = behind(d)
        got = block(core, src)
        remote(got, got, send.at[src], recv.at[src], partner).wait_recv()
        cp = remote(got, got, fsend.at[src], frecv.at[src], partner)
        cp.start()
        started.append(cp)
        if took is not None:
            took(core, src)
    for src in [chip] + [behind(d) for d in reversed(offsets)]:
        got = block(1 - core, src)
        remote(got, got, fsend.at[src], frecv.at[src], partner).wait_recv()
        if took is not None:
            took(1 - core, src)
    return started


def decode_kernel(n, pos_ref, x_ref, wq_ref, wk_ref, wv_ref, wo_ref, k_ref, v_ref, y_ref, kn_ref, vn_ref,
                  pos, x, wo, wbuf, g_ref, kbuf, vbuf, qf, kvf, raw, wts, mls, o_ref, theirs, mine, got, wcol, heads, part, ptheirs,
                  isem, wsem, ksem, asend, arecv, afsend, afrecv, xs, xr, s1, r1, s2, r2, s3, r3, send, recv, fsend, frecv):
    me, chip, core, offsets, ahead, behind = place(n)
    chips = n // 2
    partner = chip * 2 + 1 - core
    barrier = greet(core, chip, offsets, ahead)
    batch, depth = x.shape
    wide = wbuf.shape[1] // 2
    groups, per, length, kv_heads, _ = kbuf.shape
    rows = qf.shape[0] // batch
    half = batch // 2
    halves = theirs.shape[0]
    pitch = theirs.shape[1] // chips
    share = batch // halves
    base = me * length

    parts = wsem.shape[1]
    step = depth // parts

    def fetch(w_ref, block, side, j):
        return pltpu.make_async_copy(
            w_ref.at[pl.ds(j * step, step), pl.ds(pl.multiple_of(block * wide, wide), wide)],
            wbuf.at[pl.ds(j * step, step), pl.ds(side * wide, wide)], wsem.at[side, j])

    get_x = pltpu.make_async_copy(x_ref, x, isem.at[0])
    get_x.start()
    for j in range(parts):
        fetch(wq_ref, me, 0, j).start()

        @pl.when(chip < kv_heads)
        def _():
            fetch(wk_ref, chip % kv_heads, 1, j).start()

        @pl.when(chip >= kv_heads)
        def _():
            fetch(wv_ref, chip % kv_heads, 1, j).start()

    get_pos = pltpu.make_async_copy(pos_ref, pos, isem.at[1])
    get_pos.start()

    def k_in(i):
        return pltpu.make_async_copy(k_ref.at[pl.ds(i * per, per)], kbuf.at[i], ksem.at[0, i])

    def v_in(i):
        return pltpu.make_async_copy(v_ref.at[pl.ds(i * per, per)], vbuf.at[i], ksem.at[1, i])

    get_x.wait()
    acc = None
    for j in range(parts):
        fetch(wq_ref, 0, 0, j).wait()
        fetch(wk_ref, 0, 1, j).wait()
        one = jnp.dot(x[:, j * step:(j + 1) * step], wbuf[j * step:(j + 1) * step, :], preferred_element_type=F32)
        acc = one if acc is None else acc + one
    g_ref[core, chip, :batch, :] = acc[:, :wide].astype(BF16)
    kv = jnp.where(core == 0, acc[:half, wide:], acc[half:, wide:])
    g_ref[core, chip, batch:, :] = kv.astype(BF16)

    @pl.loop(0, groups)
    def _(i):
        k_in(i).start()
        v_in(i).start()

    get_wo = pltpu.make_async_copy(wo_ref, wo, isem.at[2])
    get_wo.start()
    pl.semaphore_wait(barrier, len(offsets) + 1)

    def took(c, p):
        qf[pl.ds(c * chips + p, batch, stride=rows), :] = g_ref[c, p, :batch, :].astype(F32)
        at = (p // kv_heads) * batch * kv_heads + c * half * kv_heads + p % kv_heads
        kvf[pl.ds(at, half, stride=kv_heads), :] = g_ref[c, p, batch:, :].astype(F32)

    def columns(p):
        return pl.ds(pl.multiple_of(p * 2 * wide, 2 * wide), 2 * wide)

    def spread():
        get_wo.wait()
        cps = []
        for d in offsets:
            to = ahead(d)
            cp = remote(wo.at[:, columns(to)], wcol.at[chip], s3.at[to], r3.at[chip], to * 2 + core)
            cp.start()
            cps.append(cp)
        wcol[chip] = wo[:, columns(chip)]
        return cps

    started = gather_blocks(lambda c, p: g_ref.at[c, p], chip, core, offsets, ahead, behind,
                            (asend, arecv, afsend, afrecv), took, spread)
    get_pos.wait()

    cols = length * kv_heads
    lanes = per * rows
    lane = lax.broadcasted_iota(jnp.int32, (kv_heads, lanes), 1)
    sub = lax.broadcasted_iota(jnp.int32, (kv_heads, lanes), 0)
    ours = sub == ((lane % chips) * 2 * kv_heads // rows)
    member = lane // rows
    qlane = lax.broadcasted_iota(jnp.int32, (wide, lanes), 1) // rows
    slane = lax.broadcasted_iota(jnp.int32, (rows, wide), 1)

    zero = jnp.zeros((kv_heads, 2 * wide), BF16)

    def fresh(i, j, which):
        at = (which * batch + i * per + j) * kv_heads
        return kvf[pl.ds(pl.multiple_of(at, kv_heads), kv_heads), :].astype(BF16)

    def scores(i, slot):
        k_in(i).wait()
        for j in range(per):
            kn_ref[i * per + j] = fresh(i, j, 0)
        qt = qf[pl.ds(pl.multiple_of(i * lanes, lanes), lanes), :].T.astype(BF16)
        query = jnp.concatenate([jnp.where(qlane == j, qt, 0) for j in range(per)], axis=0)
        keys = jnp.concatenate([kbuf[i, j].reshape(cols, wide) for j in range(per)], axis=1)
        raw[slot, :cols, :] = jnp.dot(keys, query, preferred_element_type=F32)
        raw[slot, cols:, :] = jnp.dot(jnp.concatenate([fresh(i, j, 0) for j in range(per)], axis=1), query,
                                      preferred_element_type=F32)

    def soften(i, slot):
        end = jnp.zeros((kv_heads, lanes), jnp.int32)
        for j in range(per):
            end = jnp.where(member == j, pos[i * per + j] - base, end)
        scale = wide ** -0.5
        t = lax.broadcasted_iota(jnp.int32, (length, kv_heads, lanes), 0)
        s = raw[slot, :cols, :].reshape(length, kv_heads, lanes) * scale
        s = jnp.where(t < jnp.where(ours, end, 0)[None], s, -jnp.inf)
        newest = jnp.where(ours & (end >= 0) & (end < length), raw[slot, cols:, :] * scale, -jnp.inf)
        m = jnp.max(jnp.maximum(jnp.max(s, axis=0), newest), axis=0, keepdims=True)
        safe = jnp.where(m == -jnp.inf, 0.0, m)
        w = jnp.exp(s - safe[None])
        nw = jnp.exp(newest - safe)
        total = jnp.sum(jnp.sum(w, axis=0) + nw, axis=0, keepdims=True)
        wts[slot, :, :cols] = w.reshape(cols, lanes).T.astype(BF16)
        wts[slot, :, cols:] = jnp.concatenate([nw, jnp.zeros((wide - kv_heads, lanes), F32)], axis=0).T.astype(BF16)
        mls[slot] = jnp.concatenate([m, total, jnp.zeros((kv_heads - 2, lanes), F32)], axis=0).T

    def values(i, slot, stats):
        v_in(i).wait()
        at = (i // (groups // halves)) * rows * pitch + (i % (groups // halves)) * per
        for j in range(0, per, 2):
            vn0, vn1 = fresh(i, j, 1), fresh(i, j + 1, 1)
            vn_ref[i * per + j] = vn0
            vn_ref[i * per + j + 1] = vn1
            vals = jnp.concatenate([vbuf[i, j].reshape(cols, wide), vbuf[i, j + 1].reshape(cols, wide)], axis=1)
            vals = jnp.concatenate([vals, jnp.concatenate([vn0, vn1], axis=1), zero], axis=0)
            o = jnp.dot(wts[slot, j * rows:(j + 2) * rows, :cols + 2 * kv_heads], vals, preferred_element_type=F32)
            o_ref[pl.ds(at + j, rows, stride=pitch), :] = o[:rows, :wide]
            o_ref[pl.ds(at + j + 1, rows, stride=pitch), :] = o[rows:, wide:]
        for j in range(per):
            z = mls[slot, j * rows:(j + 1) * rows, :]
            stats = jnp.where(slane == i * per + j, z[:, 0:1], stats)
            stats = jnp.where(slane == batch + i * per + j, z[:, 1:2], stats)
        return stats

    def attend(p, stats):
        for c in range(2):
            stats = values(2 * p + c, c, stats)
            soften(2 * p + c + 1, 1 - c)
            scores(2 * p + c + 2, c)
        return stats

    def other(v):
        return pltpu.roll(v, batch, 1)

    def swap(t):
        return remote(o_ref.at[pl.ds(pl.multiple_of((t * 2 + 1 - core) * chips * pitch, chips * pitch), chips * pitch)],
                      theirs.at[t], xs.at[t], xr.at[t], partner)

    mlane = lax.broadcasted_iota(jnp.int32, (chips, wide), 1)

    def merge_pair(t):
        swap(t).wait_recv()
        first = pl.multiple_of((t * 2 + core) * chips * pitch, chips * pitch)
        sa = o_ref[pl.ds(first + share, chips, stride=pitch), :]
        sb = theirs[t, pl.ds(share, chips, stride=pitch), :]
        m = jnp.maximum(sa, sb)
        safe = jnp.where(m == -jnp.inf, 0.0, m)
        wa, wb = jnp.exp(sa - safe), jnp.exp(sb - safe)
        total = other(sa) * wa + other(sb) * wb
        mine[t, pl.ds(share, chips, stride=pitch), :] = jnp.where(mlane < batch, m, other(total))
        wt = jnp.concatenate([wa, wb], axis=0).T
        mid = slice(t * share, (t + 1) * share)
        for p in range(chips):
            a = o_ref[pl.ds(first + p * pitch, share), :] * wt[mid, p:p + 1]
            b = theirs[t, p * pitch:p * pitch + share, :] * wt[mid, chips + p:chips + p + 1]
            mine[t, p * pitch:p * pitch + share, :] = a + b
        for d in offsets:
            to = ahead(d)
            cp = remote(used(mine.at[t], to), used(got.at[t], chip), s1.at[t, to], r1.at[t, chip], to * 2 + core)
            cp.start()
            started.append(cp)
        own = pl.ds(pl.multiple_of(chip * pitch, pitch), pitch)
        got[t, own, :] = mine[t, own, :]

    def slot(ref, p):
        size = ref.shape[0] // chips
        return ref.at[pl.ds(pl.multiple_of(p * size, size), size)]

    def used(ref, p):
        return ref.at[pl.ds(pl.multiple_of(p * pitch, pitch), share + 1)]

    def merge_chips(t):
        for d in offsets:
            src = behind(d)
            remote(used(got.at[t], src), used(got.at[t], src), s1.at[t, src], r1.at[t, src], partner).wait_recv()
        s = got[t, pl.ds(share, chips, stride=pitch), :]
        w = jnp.exp(s - jnp.max(s, axis=0, keepdims=True))
        w = w / jnp.sum(other(s) * w, axis=0, keepdims=True)
        wt = w.T
        mid = slice(t * share, (t + 1) * share)
        out = got[t, :share, :] * wt[mid, 0:1]
        for p in range(1, chips):
            out = out + got[t, p * pitch:p * pitch + share, :] * wt[mid, p:p + 1]
        return out.astype(BF16)

    pairs = groups // 2
    none = jnp.zeros((rows, wide), F32)
    scores(0, 0)
    soften(0, 0)
    scores(1, 1)

    def finish(t, stats):
        o_ref[pl.ds(t * rows * pitch + share, rows, stride=pitch), :] = stats
        swap(t).start()

    finish(0, lax.fori_loop(0, pairs // 2, attend, none))
    stats = lax.fori_loop(pairs // 2, pairs - 1, attend, none)
    merge_pair(0)
    stats = values(groups - 2, 0, stats)
    soften(groups - 1, 1)
    finish(1, values(groups - 1, 1, stats))
    merge_pair(1)
    out = jnp.concatenate([merge_chips(t) for t in range(halves)], axis=0)
    heads[chip] = out
    for d in offsets:
        to = ahead(d)
        cp = remote(heads.at[chip], heads.at[chip], s2.at[to], r2.at[chip], to * 2 + core)
        cp.start()
        started.append(cp)
    for d in offsets:
        src = behind(d)
        remote(wcol.at[src], wcol.at[src], s3.at[src], r3.at[src], partner).wait_recv()
    for d in offsets:
        src = behind(d)
        remote(heads.at[src], heads.at[src], s2.at[src], r2.at[src], partner).wait_recv()
    y = jnp.dot(jnp.concatenate([heads[p] for p in range(chips)], axis=1), wcol[...].reshape(chips * wide, 2 * wide),
                preferred_element_type=F32)
    part[0] = y[:, :wide]
    part[1] = y[:, wide:]
    swap2 = remote(part.at[1 - core], ptheirs, xs.at[halves], xr.at[halves], partner)
    swap2.start()
    swap2.wait_recv()
    y = part[core] + ptheirs[...]
    y_ref[:, pl.ds(pl.multiple_of(me * wide, wide), wide)] = y.astype(BF16)

    def block(c, p):
        return y_ref.at[:, pl.ds(pl.multiple_of((p * 2 + c) * wide, wide), wide)]

    started += gather_blocks(block, chip, core, offsets, ahead, behind, (send, recv, fsend, frecv))
    for t in range(halves):
        swap(t).wait_send()
    swap2.wait_send()
    for cp in started:
        cp.wait_send()


def store_kernel(pos_hbm, k_ref, v_ref, kn_ref, vn_ref, y_ref, ko_ref, vo_ref, yo_ref, pos_ref, sem, rsem, ysem):
    batch, length = k_ref.shape[:2]
    chunks = sem.shape[1]
    per = batch // chunks
    base = lax.axis_index('seq') * length

    def whole(src, dst, a, i):
        return pltpu.make_async_copy(src.at[pl.ds(i * per, per)], dst.at[pl.ds(i * per, per)], sem.at[a, i])

    def row(src, dst, a, b):
        at = jnp.clip(pos_ref[b] - base, 0, length - 1)
        return pltpu.make_async_copy(src.at[b], dst.at[b, at], rsem.at[a, b])

    def here(b):
        end = pos_ref[b] - base
        return (end >= 0) & (end < length)

    @pl.loop(0, chunks)
    def _(i):
        whole(k_ref, ko_ref, 0, i).start()
        whole(v_ref, vo_ref, 1, i).start()

    y = pltpu.make_async_copy(y_ref, yo_ref, ysem.at[0])
    y.start()
    get_pos = pltpu.make_async_copy(pos_hbm, pos_ref, ysem.at[1])
    get_pos.start()
    get_pos.wait()

    @pl.loop(0, chunks)
    def _(i):
        whole(k_ref, ko_ref, 0, i).wait()
        whole(v_ref, vo_ref, 1, i).wait()
        for j in range(per):
            b = i * per + j

            @pl.when(here(b))
            def _():
                row(kn_ref, ko_ref, 0, b).start()
                row(vn_ref, vo_ref, 1, b).start()

    y.wait()

    @pl.loop(0, batch)
    def _(b):
        @pl.when(here(b))
        def _():
            row(kn_ref, ko_ref, 0, b).wait()
            row(vn_ref, vo_ref, 1, b).wait()


def solution(mesh):
    n = mesh.shape['seq']
    chips = n // 2
    cache_spec = P('rep', 'seq', None, None)
    in_specs = (P('rep', None), P(), P(), P(), P('seq', None), cache_spec, cache_spec, P('rep'))
    out_specs = (P('rep', None), cache_spec, cache_spec)
    vmem = pl.BlockSpec(memory_space=pltpu.VMEM)
    smem = pl.BlockSpec(memory_space=pltpu.SMEM)
    hbm = pl.BlockSpec(memory_space=pltpu.HBM)
    anywhere = pl.BlockSpec(memory_space=pl.ANY)

    def step(x, wq, wk, wv, wo, k, v, pos):
        batch, depth = x.shape
        length, kv_heads, wide = k.shape[1:]
        heads = wq.shape[1] // wide
        slots = DMA((chips,))
        per = 2 * wide // heads
        groups = batch // per
        halves = 2
        pitch = batch // halves + 8
        cache = VMEM((groups, per, length, kv_heads, wide), BF16)
        new = jax.ShapeDtypeStruct((batch, kv_heads, wide), BF16)
        y, kn, vn = pl.pallas_call(
            functools.partial(decode_kernel, n),
            out_shape=[jax.ShapeDtypeStruct((batch, depth), BF16), new, new],
            in_specs=[anywhere] * 8, out_specs=[vmem] * 3,
            scratch_shapes=[
                pltpu.SMEM((batch,), jnp.int32), VMEM((batch, depth), BF16), VMEM(wo.shape, BF16),
                VMEM((depth, 2 * wide), BF16), VMEM((2, chips, batch + batch // 2, wide), BF16), cache, cache,
                VMEM((batch * heads, wide), F32), VMEM((2 * batch * kv_heads, wide), F32),
                VMEM((2, (length + 1) * kv_heads, per * heads), F32),
                VMEM((2, per * heads, length * kv_heads + wide), BF16), VMEM((2, per * heads, kv_heads), F32),
                VMEM((halves * heads * pitch, wide), F32)]
            + [VMEM((halves, chips * pitch, wide), F32)] * 3
            + [VMEM((chips, wide, 2 * wide), BF16), VMEM((chips, batch, wide), BF16), VMEM((2, batch, wide), F32),
               VMEM((batch, wide), F32)] + [DMA((3,)), DMA((2, 1)), DMA((2, groups))] + [slots] * 4
            + [DMA((halves + 1,))] * 2 + [DMA((halves, chips))] * 2 + [slots] * 8,
            compiler_params=pltpu.CompilerParams(collective_id=0, has_side_effects=True, vmem_limit_bytes=45 << 20),
            cost_estimate=pl.CostEstimate(flops=10 ** 10, bytes_accessed=32 << 20, transcendentals=0),
            name='decode',
        )(*(pltpu.with_memory_space_constraint(a, pltpu.HBM) for a in (pos, x, wq, wk, wv, wo, k, v)))
        chunks = 4
        ko, vo, y = pl.pallas_call(
            store_kernel,
            out_shape=[jax.ShapeDtypeStruct(k.shape, k.dtype), jax.ShapeDtypeStruct(v.shape, v.dtype),
                       jax.ShapeDtypeStruct((batch, depth), BF16)],
            in_specs=[anywhere, anywhere, anywhere, vmem, vmem, vmem], out_specs=[hbm, hbm, hbm],
            scratch_shapes=[pltpu.SMEM((batch,), jnp.int32), DMA((2, chunks)), DMA((2, batch)), DMA((2,))],
            compiler_params=pltpu.CompilerParams(vmem_limit_bytes=4 << 20),
            cost_estimate=pl.CostEstimate(flops=10 ** 8, bytes_accessed=32 << 20, transcendentals=0),
            name='store',
        )(pos, k, v, kn, vn, y)
        return y, ko, vo

    return jax.shard_map(step, mesh=mesh, in_specs=in_specs, out_specs=out_specs, check_vma=False)
```
